128 devices in a mesh: tp: 2 (over core), dp: 64 (over z, y, x).
Axes of the slice: x: 4, y: 4, z: 4, core: 2. Of those that a mesh axis runs over, the one named last changes fastest.
Arguments:
- hidden: bfloat16 [64, 1024, 576], P('dp')
- norm_w: bfloat16 [576], replicated
- embed: bfloat16 [49152, 576], P('tp')
- targets: int32 [64, 1024], P('dp')
- loss_mask: int32 [64, 1024], P('dp')
- token_ids: int32 [64, 1024], P('dp')
- grad_embed: bfloat16 [64, 1024, 576], P('dp')
Outputs:
- output 1: float32 [], replicated
- output 2: bfloat16 [64, 1024, 576], P('dp')
- output 3: float32 [576], replicated
- output 4: float32 [49152, 576], P('tp', 'dp')
All inputs are finite; a program needn't handle non-finite values.
Results may differ from the reference program's by a relative error of at most 0.001.
Values sent between devices are 32-bit elements.
A program may use at most 1 GiB of HBM per device.

```python
import jax
import jax.numpy as jnp
from jax import lax

VOCAB_SIZE = 49152
D_MODEL = 576
BATCH_SIZE = 64
SEQ_LEN = 1024
ROW_BLOCK = 128
RMS_EPS = 1e-6


def skewed_ids(rand_key, shape):
    key_a, key_b, key_c = jax.random.split(rand_key, 3)
    first = jax.random.randint(key_a, shape, 0, VOCAB_SIZE)
    second = jax.random.randint(key_b, shape, 0, first + 1)
    return jax.random.randint(key_c, shape, 0, second + 1).astype(jnp.int32)


def setup_inputs(seed: int = 0) -> dict:
    key_list = jax.random.split(jax.random.key(seed), 8)
    tokens = BATCH_SIZE * SEQ_LEN
    hidden = jax.random.normal(key_list[0], (BATCH_SIZE, SEQ_LEN, D_MODEL), jnp.float32)
    norm_w = 1.0 + 0.3 * jax.random.normal(key_list[1], (D_MODEL,), jnp.float32)
    embed = (1.5 / D_MODEL ** 0.5) * jax.random.normal(key_list[2], (VOCAB_SIZE, D_MODEL), jnp.float32)
    targets = skewed_ids(key_list[3], (BATCH_SIZE, SEQ_LEN))
    token_ids = skewed_ids(key_list[4], (BATCH_SIZE, SEQ_LEN))
    lengths = jax.random.randint(key_list[5], (BATCH_SIZE, 1), SEQ_LEN // 4, SEQ_LEN + 1)
    loss_mask = (jnp.arange(SEQ_LEN)[None, :] < lengths).astype(jnp.int32)
    grad_embed = (1.5 / tokens) * jax.random.normal(key_list[6], (BATCH_SIZE, SEQ_LEN, D_MODEL), jnp.float32)
    return {"hidden": hidden.astype(jnp.bfloat16), "norm_w": norm_w.astype(jnp.bfloat16), "embed": embed.astype(jnp.bfloat16), "targets": targets, "loss_mask": loss_mask, "token_ids": token_ids, "grad_embed": grad_embed.astype(jnp.bfloat16)}


def reference(hidden, norm_w, embed, targets, loss_mask, token_ids, grad_embed):
    tokens = BATCH_SIZE * SEQ_LEN
    blocks = tokens // ROW_BLOCK
    hidden32 = hidden.reshape(tokens, D_MODEL).astype(jnp.float32)
    norm_gain = norm_w.astype(jnp.float32)

    def rms_norm(rows, weight):
        inv_rms = lax.rsqrt(jnp.mean(rows * rows, axis=-1, keepdims=True) + RMS_EPS)
        return rows * inv_rms * weight

    normed, norm_vjp = jax.vjp(rms_norm, hidden32, norm_gain)
    z_rows = normed.astype(jnp.bfloat16)
    mask_rows = loss_mask.reshape(tokens).astype(jnp.float32)
    token_count = jnp.sum(mask_rows)
    vocab_index = jnp.arange(VOCAB_SIZE)

    def block_step(grad_accum, block_in):
        z_block, target_block, mask_block = block_in
        logits = jnp.dot(z_block, embed.T, preferred_element_type=jnp.float32)
        row_max = jnp.max(logits, axis=-1, keepdims=True)
        log_norm = row_max + jnp.log(jnp.sum(jnp.exp(logits - row_max), axis=-1, keepdims=True))
        is_target = vocab_index[None, :] == target_block[:, None]
        target_logit = jnp.sum(jnp.where(is_target, logits, 0.0), axis=-1, keepdims=True)
        soft_probs = jnp.exp(logits - log_norm)
        dlogits = ((soft_probs - is_target.astype(jnp.float32)) * (mask_block[:, None] / token_count)).astype(jnp.bfloat16)
        grad_z = jnp.dot(dlogits, embed, preferred_element_type=jnp.float32)
        grad_accum = grad_accum + jnp.dot(dlogits.T, z_block, preferred_element_type=jnp.float32)
        loss_part = jnp.sum(mask_block * (log_norm[:, 0] - target_logit[:, 0]))
        return grad_accum, (grad_z, loss_part)

    block_inputs = (z_rows.reshape(blocks, ROW_BLOCK, D_MODEL), targets.reshape(blocks, ROW_BLOCK), mask_rows.reshape(blocks, ROW_BLOCK))
    head_grad, (grad_z_blocks, loss_parts) = lax.scan(block_step, jnp.zeros((VOCAB_SIZE, D_MODEL), jnp.float32), block_inputs)
    grad_z = grad_z_blocks.reshape(tokens, D_MODEL)
    grad_hidden32, grad_gain = norm_vjp(grad_z)
    lookup_grad = jax.ops.segment_sum(grad_embed.reshape(tokens, D_MODEL).astype(jnp.float32), token_ids.reshape(tokens), num_segments=VOCAB_SIZE)
    loss_val = jnp.sum(loss_parts) / token_count
    grad_hidden = grad_hidden32.astype(jnp.bfloat16).reshape(BATCH_SIZE, SEQ_LEN, D_MODEL)
    return (loss_val, grad_hidden, grad_gain, head_grad + lookup_grad)
```

```python
import functools

import jax
import jax.numpy as jnp
from jax import lax
from jax.experimental import pallas as pl
from jax.experimental.pallas import tpu as pltpu
from jax.sharding import Mesh, PartitionSpec as P

RMS_EPS = 1e-6
F32, BF16, I32 = jnp.float32, jnp.bfloat16, jnp.int32
D = 576
TOK = 1024
GX = 4
TT = GX * TOK
VL = 24576
VB = VL // GX
TS = 512
NS = TT // TS
V2 = 256
N2 = VB // V2
TB = 256
CH = 256
VMEM = pl.BlockSpec(memory_space=pltpu.VMEM)
ANY = pl.BlockSpec(memory_space=pl.ANY)


def prep_kernel(h_ref, ge_ref, w_ref, zf_ref, gf_ref):
    rows = h_ref[...].astype(F32)
    inv = lax.rsqrt(jnp.mean(rows * rows, axis=0, keepdims=True) + RMS_EPS)
    z = (rows * inv * w_ref[...].astype(F32)).astype(BF16)
    zf_ref[...] = z.astype(F32)
    gf_ref[...] = ge_ref[...].astype(F32)


def prep(h_t, ge_t, w):
    return pl.pallas_call(
        prep_kernel,
        out_shape=(jax.ShapeDtypeStruct((D, TOK), F32), jax.ShapeDtypeStruct((D, TOK), F32)),
        in_specs=[VMEM, VMEM, VMEM],
        out_specs=(VMEM, VMEM),
        compiler_params=pltpu.CompilerParams(vmem_limit_bytes=40 << 20),
    )(h_t, ge_t, w)


def forward_kernel(et_ref, zg_ref, tgt_ref, logit_ref, stat_ref, zb_ref, gb_ref, e_s, stage, ebuf, fbuf, esem, osem, fsem):
    vstart = lax.axis_index("x") * VB

    def ecopy(i, slot):
        cols = pl.ds(pl.multiple_of(vstart + i * 512, 128), 512)
        return pltpu.make_async_copy(et_ref.at[:, cols], ebuf.at[slot], esem.at[slot])

    def fcopy(i, slot):
        return pltpu.make_async_copy(zg_ref.at[i // 2, i % 2], fbuf.at[slot], fsem.at[slot])

    fcopy(0, 0).start()
    ecopy(0, 0).start()
    for i in range(2 * NS):
        if i + 1 < 2 * NS:
            fcopy(i + 1, (i + 1) % 2).start()
        fcopy(i, i % 2).wait()
        dst = zb_ref if i % 2 == 0 else gb_ref
        dst[i // 2] = fbuf[i % 2].astype(BF16)

    def ebody(i, _):
        slot = lax.rem(i, 2)

        @pl.when(i + 1 < VB // 512)
        def _():
            ecopy(i + 1, 1 - slot).start()

        ecopy(i, slot).wait()
        e_s[pl.ds(pl.multiple_of(i * 512, 512), 512), :] = ebuf[slot].T
        return 0

    lax.fori_loop(0, VB // 512, ebody, 0)
    iota = lax.broadcasted_iota(I32, (8, TB), 0)

    def ocopy(ts, half, slot):
        return pltpu.make_async_copy(stage.at[slot], logit_ref.at[ts, :, pl.ds(half * TB, TB)], osem.at[slot])

    def ts_body(ts, _):
        for half in range(2):
            @pl.when(ts > 0)
            def _():
                ocopy(ts, half, half).wait()

            lanes = slice(half * TB, half * TB + TB)
            zt = zb_ref[ts, :, lanes]
            tgt = tgt_ref[ts, 0:1, lanes] - vstart
            m8 = jnp.full((8, TB), -jnp.inf, F32)
            s8 = jnp.zeros((8, TB), F32)
            t8 = jnp.zeros((8, TB), F32)
            for vc in range(VB // CH):
                l = jnp.dot(e_s[vc * CH:(vc + 1) * CH, :], zt, preferred_element_type=F32)
                stage[half, vc * CH:(vc + 1) * CH, :] = l
                mn = m8
                for r in range(CH // 8):
                    mn = jnp.maximum(mn, l[r * 8:r * 8 + 8])
                s8 = s8 * jnp.exp(m8 - mn)
                m8 = mn
                for r in range(CH // 8):
                    lr = l[r * 8:r * 8 + 8]
                    s8 = s8 + jnp.exp(lr - mn)
                    t8 = t8 + jnp.where(iota == tgt - (vc * CH + r * 8), lr, 0.0)
            m = jnp.max(m8, axis=0, keepdims=True)
            stat_ref[ts, 0:1, lanes] = m
            stat_ref[ts, 1:2, lanes] = jnp.sum(s8 * jnp.exp(m8 - m), axis=0, keepdims=True)
            stat_ref[ts, 2:3, lanes] = jnp.sum(t8, axis=0, keepdims=True)
            ocopy(ts, half, half).start()
        return 0

    lax.fori_loop(0, NS, ts_body, 0)
    for half in range(2):
        ocopy(0, half, half).wait()


def forward(et, zg, tgt):
    return pl.pallas_call(
        forward_kernel,
        out_shape=(
            jax.ShapeDtypeStruct((NS, VB, TS), F32),
            jax.ShapeDtypeStruct((NS, 8, TS), F32),
            jax.ShapeDtypeStruct((NS, D, TS), BF16),
            jax.ShapeDtypeStruct((NS, D, TS), BF16),
        ),
        in_specs=[ANY, ANY, VMEM],
        out_specs=(ANY, VMEM, VMEM, VMEM),
        scratch_shapes=[
            pltpu.VMEM((VB, D), BF16),
            pltpu.VMEM((2, VB, TB), F32),
            pltpu.VMEM((2, D, 512), BF16),
            pltpu.VMEM((2, D, TS), F32),
            pltpu.SemaphoreType.DMA((2,)),
            pltpu.SemaphoreType.DMA((2,)),
            pltpu.SemaphoreType.DMA((2,)),
        ],
        compiler_params=pltpu.CompilerParams(vmem_limit_bytes=60 << 20),
    )(et, zg, tgt)


def backward_kernel(et_ref, zt_ref, gt_ref, row_ref, ids_ref, logit_ref, dz_ref, de_ref, lbuf, et_s, lsem, esem):
    vstart = lax.axis_index("x") * VB
    iota = lax.broadcasted_iota(I32, (V2, TS), 0)

    def lcopy(vc, slot):
        return pltpu.make_async_copy(logit_ref.at[:, pl.ds(vc * V2, V2), :], lbuf.at[slot], lsem.at[slot])

    def ecopy(vc, slot):
        cols = pl.ds(pl.multiple_of(vstart + vc * V2, 128), V2)
        return pltpu.make_async_copy(et_ref.at[:, cols], et_s.at[slot], esem.at[slot])

    for slot in range(2):
        lcopy(slot, slot).start()
        ecopy(slot, slot).start()
    dz_ref[...] = jnp.zeros_like(dz_ref)

    def v_body(vc, _):
        slot = lax.rem(vc, 2)
        lcopy(vc, slot).wait()
        ecopy(vc, slot).wait()
        et = et_s[slot]
        base = vstart + vc * V2
        acc = jnp.zeros((D, V2), F32)
        for ts in range(NS):
            p = jnp.exp(lbuf[slot, ts] - row_ref[ts, 0:1, :])
            d = (jnp.where(iota == ids_ref[ts, 0:1, :] - base, p - 1.0, p) * row_ref[ts, 1:2, :]).astype(BF16)
            dz_ref[ts] += jnp.dot(et, d, preferred_element_type=F32)
            acc += lax.dot_general(zt_ref[ts], d, (((1,), (1,)), ((), ())), preferred_element_type=F32)
            o = jnp.where(iota == ids_ref[ts, 1:2, :] - base, 1.0, 0.0).astype(BF16)
            acc += lax.dot_general(gt_ref[ts], o, (((1,), (1,)), ((), ())), preferred_element_type=F32)
        de_ref[vc] = acc
        nxt = jnp.minimum(vc + 2, N2 - 1)
        lcopy(nxt, slot).start()
        ecopy(nxt, slot).start()
        return 0

    lax.fori_loop(0, N2, v_body, 0)
    for slot in range(2):
        lcopy(0, slot).wait()
        ecopy(0, slot).wait()


def backward(et, zb, gb, row, ids, logit):
    return pl.pallas_call(
        backward_kernel,
        out_shape=(jax.ShapeDtypeStruct((NS, D, TS), F32), jax.ShapeDtypeStruct((N2, D, V2), F32)),
        in_specs=[ANY, VMEM, VMEM, VMEM, VMEM, ANY],
        out_specs=(VMEM, VMEM),
        scratch_shapes=[
            pltpu.VMEM((2, NS, V2, TS), F32),
            pltpu.VMEM((2, D, V2), BF16),
            pltpu.SemaphoreType.DMA((2,)),
            pltpu.SemaphoreType.DMA((2,)),
        ],
        compiler_params=pltpu.CompilerParams(vmem_limit_bytes=63 << 20),
    )(et, zb, gb, row, ids, logit)


def solution(mesh):
    mesh4 = Mesh(mesh.devices.reshape(2, 4, 4, 4), ("tp", "z", "y", "x"))

    def local_step(hidden, norm_w, embed, targets, loss_mask, token_ids, grad_embed):
        core, xi = lax.axis_index("tp"), lax.axis_index("x")
        h_t = hidden.reshape(TOK, D).T
        ge_t = grad_embed.reshape(TOK, D).T
        et = embed.T
        zf, gf = prep(h_t, ge_t, norm_w.reshape(D, 1))
        both = jnp.stack([zf, gf])
        half = lax.dynamic_slice(both, (0, 0, core * TS), (2, D, TS))
        zg = lax.all_gather(half, ("x", "tp"), axis=0)
        ints = jnp.stack([targets.reshape(TOK), token_ids.reshape(TOK), loss_mask.reshape(TOK)])
        ints_g = lax.all_gather(ints, "x", axis=0)
        ints_g = ints_g.reshape(GX, 3, 2, TS).transpose(0, 2, 1, 3).reshape(NS, 3, TS)
        ids = jnp.pad(ints_g[:, :2] - core * VL, ((0, 0), (0, 6), (0, 0)))
        logit, stat, zb, gb = forward(et, zg, ids)
        stats = lax.all_gather(stat[:, :3], ("tp", "x"), axis=0)
        m = jnp.max(stats[:, :, 0], axis=0)
        s = jnp.sum(stats[:, :, 1] * jnp.exp(stats[:, :, 0] - m), axis=0)
        lse = m + jnp.log(s)
        tgt_logit = jnp.sum(stats[:, :, 2], axis=0)
        mask_own = loss_mask.reshape(TOK).astype(F32)
        lse_own = lax.dynamic_slice(lse, (2 * xi, 0), (2, TS)).reshape(TOK)
        tgt_own = lax.dynamic_slice(tgt_logit, (2 * xi, 0), (2, TS)).reshape(TOK)
        sums = lax.psum(jnp.stack([jnp.sum(mask_own), jnp.sum(mask_own * (lse_own - tgt_own))]), ("tp", "z", "y", "x")) * 0.5
        count = sums[0]
        loss_val = sums[1] / count
        scale = ints_g[:, 2].astype(F32) / count
        row = jnp.pad(jnp.stack([lse, scale], axis=1), ((0, 0), (0, 6), (0, 0)))
        dz, de = backward(et, zb, gb, row, ids, logit)
        dz = lax.psum_scatter(dz.reshape(GX, 2, D, TS), "x", scatter_dimension=0, tiled=True)
        dz = lax.psum(dz, "tp").reshape(2, D, TS).transpose(1, 0, 2).reshape(D, TOK)
        de = de.transpose(1, 0, 2).reshape(D, 16, VB // 16).transpose(1, 0, 2)
        de = lax.psum_scatter(de, ("z", "y"), scatter_dimension=0, tiled=True)
        de = lax.all_to_all(de.reshape(64, 9, VB // 16), ("z", "y", "x"), 0, 0)
        de = de.reshape(16, GX, 9, VB // 16).transpose(2, 1, 0, 3).reshape(9, VL)
        rows = h_t.astype(F32)
        inv = lax.rsqrt(jnp.mean(rows * rows, axis=0, keepdims=True) + RMS_EPS)
        unit = rows * inv
        grad_gain = lax.psum(jnp.sum(dz * unit, axis=1), ("tp", "z", "y", "x")) * 0.5
        gu = dz * norm_w.astype(F32).reshape(D, 1)
        grad_hidden = inv * (gu - unit * jnp.mean(gu * unit, axis=0, keepdims=True))
        grad_hidden = grad_hidden.astype(BF16).T.reshape(1, TOK, D)
        return loss_val, grad_hidden, grad_gain, de.T

    dp = ("z", "y", "x")
    return jax.shard_map(
        local_step,
        mesh=mesh4,
        in_specs=(P(dp), P(), P("tp"), P(dp), P(dp), P(dp), P(dp)),
        out_specs=(P(), P(dp), P(), P("tp", dp)),
        check_vma=False,
    )
```

```python
import functools

import jax
import jax.numpy as jnp
from jax import lax
from jax.experimental import pallas as pl
from jax.experimental.pallas import tpu as pltpu
from jax.sharding import Mesh, PartitionSpec as P

RMS_EPS = 1e-6
F32, BF16, I32 = jnp.float32, jnp.bfloat16, jnp.int32
MESH = pl.DeviceIdType.MESH
D = 576
TOK = 1024
GX = 4
VL = 24576
VB = VL // GX
TS = 512
TB = 256
NS = GX * 2
V2 = 256
N2 = VB // V2
CH = 256
VMEM = pl.BlockSpec(memory_space=pltpu.VMEM)
ANY = pl.BlockSpec(memory_space=pl.ANY)
DELTA = (0, 3, 1, 2)
SLOT = {0: 0, 3: 1, 1: 2, 2: 3}


def remote(src, dst, send, recv, where):
    return pltpu.make_async_remote_copy(src_ref=src, dst_ref=dst, send_sem=send, recv_sem=recv, device_id=where, device_id_type=MESH)


def forward_kernel(
    h_ref, ge_ref, w_ref, ints_ref, et_ref,
    logit_ref, zb_out, uf_out, gf_out, row_ref, ids_ref, aux_ref,
    e_s, stage, ebuf, uf, zb, ints, stats, ny, nz,
    esem, osem, zsem, fsem, usend, urecv, psend, precv, isend, irecv, ssend, srecv, nsend, nrecv,
):
    core = lax.axis_index("tp")
    xi, yi, zi = lax.axis_index("x"), lax.axis_index("y"), lax.axis_index("z")
    other = 1 - core

    def at_x(d):
        return lax.rem(xi + d, 4)

    right, left = at_x(1), at_x(3)
    vstart = xi * VB

    def ecopy(i, slot):
        cols = pl.ds(pl.multiple_of(vstart + i * 512, 128), 512)
        return pltpu.make_async_copy(et_ref.at[:, cols], ebuf.at[slot], esem.at[slot])

    ecopy(0, 0).start()
    barrier = pltpu.get_barrier_semaphore()
    peers = [{"x": at_x(d)} for d in (1, 2, 3)] + [{"x": at_x(d), "tp": other} for d in range(4)]
    peers += [{"y": lax.rem(yi + d, 4)} for d in (1, 2, 3)] + [{"z": lax.rem(zi + d, 4)} for d in (1, 2, 3)]
    for peer in peers:
        pl.semaphore_signal(barrier, inc=1, device_id=peer, device_id_type=MESH)

    ints[0] = ints_ref[...]
    weight = w_ref[...].astype(F32)
    for half in range(2):
        for q in range(2):
            lo = half * TS + q * TB
            rows = h_ref[:, lo:lo + TB].astype(F32)
            inv = lax.rsqrt(jnp.mean(rows * rows, axis=0, keepdims=True) + RMS_EPS)
            uf[half, q] = rows * inv
    for q in range(2):
        lo = q * TB
        gf_out[q] = jnp.where(core == 0, ge_ref[:, lo:lo + TB].astype(F32), ge_ref[:, TS + lo:TS + lo + TB].astype(F32))
    pl.semaphore_wait(barrier, len(peers))

    def ucopy(src, q, dst, way, index):
        return remote(uf.at[2 * src + core, q], uf.at[2 * dst + core, q], usend.at[index], urecv.at[dst, q], {"x": way})

    def pcopy(r, q):
        return remote(uf.at[2 * r + core, q], uf.at[2 * r + core, q], psend.at[r, q], precv.at[r, q], {"tp": other})

    def parrive(r, q):
        return remote(uf.at[2 * r + core, q], uf.at[2 * r + other, q], psend.at[r, q], precv.at[r, q], {"tp": other})

    own = [ucopy(0, 0, 1, right, 0), ucopy(0, 0, 2, left, 1), ucopy(0, 1, 1, right, 2), ucopy(0, 1, 2, left, 3)]
    onward = [ucopy(1, 0, 3, right, 4), ucopy(2, 1, 3, left, 5)]

    def icopy(d):
        return remote(ints.at[0], ints.at[SLOT[(4 - d) % 4]], isend.at[d], irecv.at[SLOT[(4 - d) % 4]], {"x": at_x(d)})

    for copy in own[:2]:
        copy.start()
    for d in (1, 2, 3):
        icopy(d).start()
    for copy in own[2:]:
        copy.start()

    def ebody(i, _):
        slot = lax.rem(i, 2)

        @pl.when(i + 1 < VB // 512)
        def _():
            ecopy(i + 1, 1 - slot).start()

        ecopy(i, slot).wait()
        e_s[pl.ds(pl.multiple_of(i * 512, 512), 512), :] = ebuf[slot].T
        return 0

    lax.fori_loop(0, VB // 512, ebody, 0)

    def scopy(r, d, cross):
        index = 2 * d + cross
        where = {"x": at_x(d), "tp": other} if cross else {"x": at_x(d)}
        dst = SLOT[(DELTA[r] - d) % 4]
        return remote(stats.at[0, r], stats.at[index, dst], ssend.at[index, r], srecv.at[index, dst], where)

    def stat_copies(r):
        return [scopy(r, d, cross) for d in range(4) for cross in range(2) if d or cross]

    def ncopy(buf, axis, me, d):
        k = {"y": 0, "z": 1}[axis]
        return remote(buf.at[me], buf.at[me], nsend.at[k, d], nrecv.at[k, d], {axis: lax.rem(me + d, 4)})

    def narrive(buf, axis, me, d):
        k = {"y": 0, "z": 1}[axis]
        return remote(buf.at[me], buf.at[lax.rem(me + 4 - d, 4)], nsend.at[k, d], nrecv.at[k, d], {axis: lax.rem(me + d, 4)})

    iota = lax.broadcasted_iota(I32, (8, TB), 0)

    def ocopy(ts, q, slot):
        return pltpu.make_async_copy(stage.at[slot], logit_ref.at[ts, :, pl.ds(pl.multiple_of(q * TB, TB), TB)], osem.at[slot])

    def zcopy(ts, q):
        return pltpu.make_async_copy(zb.at[ts, q], zb_out.at[ts, q], zsem.at[ts, q])

    def fcopy(ts, q):
        return pltpu.make_async_copy(uf.at[ts, q], uf_out.at[ts, q], fsem.at[ts, q])

    def step(s, _):
        k, j = (s - 4) // 4, lax.rem(s, 4)
        r = jnp.where(s < 4, 0, jnp.where(s < 12, 1 + lax.rem(j, 2), 3))
        q = jnp.where(s < 4, lax.rem(j, 2), jnp.where(s < 12, k, lax.rem(j, 2)))
        half = jnp.where(s < 4, j // 2, jnp.where(j < 2, core, other))
        ts = 2 * r + half

        @pl.when(s == 4)
        def _():
            own[0].wait_recv()
            onward[0].start()
            pcopy(1, 0).start()
            own[1].wait_recv()
            pcopy(2, 0).start()
            for d in (1, 2, 3):
                icopy(d).wait_recv()
            for copy in stat_copies(0):
                copy.start()

        @pl.when(s == 6)
        def _():
            parrive(1, 0).wait_recv()
            parrive(2, 0).wait_recv()

        @pl.when(s == 8)
        def _():
            own[3].wait_recv()
            onward[1].start()
            pcopy(2, 1).start()
            own[2].wait_recv()
            pcopy(1, 1).start()
            count = jnp.sum(ints[:, :, :, 2, :].astype(F32))
            ny[yi] = jnp.full((8, 128), count, F32)
            for d in (1, 2, 3):
                ncopy(ny, "y", yi, d).start()

        @pl.when(s == 10)
        def _():
            parrive(1, 1).wait_recv()
            parrive(2, 1).wait_recv()
            for d in (1, 2, 3):
                narrive(ny, "y", yi, d).wait_recv()
            nz[zi] = ny[0] + ny[1] + ny[2] + ny[3]
            for d in (1, 2, 3):
                ncopy(nz, "z", zi, d).start()

        @pl.when(s == 12)
        def _():
            onward[0].wait_recv()
            pcopy(3, 0).start()
            onward[1].wait_recv()
            pcopy(3, 1).start()
            for copy in stat_copies(1) + stat_copies(2):
                copy.start()

        @pl.when(s == 14)
        def _():
            parrive(3, 0).wait_recv()
            parrive(3, 1).wait_recv()

        slot = lax.rem(s, 2)

        @pl.when(s >= 2)
        def _():
            ocopy(ts, q, slot).wait()

        zt = (uf[ts, q] * weight).astype(BF16)
        zb[ts, q] = zt
        zcopy(ts, q).start()
        fcopy(ts, q).start()
        tgt = ints[r, half, q, 0:1, :] - vstart
        m8 = jnp.full((8, TB), -jnp.inf, F32)
        s8 = jnp.zeros((8, TB), F32)
        t8 = jnp.zeros((8, TB), F32)
        for vc in range(VB // CH):
            l = jnp.dot(e_s[vc * CH:(vc + 1) * CH, :], zt, preferred_element_type=F32)
            stage[slot, vc * CH:(vc + 1) * CH, :] = l
            mn = m8
            for i in range(CH // 8):
                mn = jnp.maximum(mn, l[i * 8:i * 8 + 8])
            s8 = s8 * jnp.exp(m8 - mn)
            m8 = mn
            for i in range(CH // 8):
                li = l[i * 8:i * 8 + 8]
                s8 = s8 + jnp.exp(li - mn)
                t8 = t8 + jnp.where(iota == tgt - (vc * CH + i * 8), li, 0.0)
        m = jnp.max(m8, axis=0, keepdims=True)
        stats[0, r, half, q, 0:1, :] = m
        stats[0, r, half, q, 1:2, :] = jnp.sum(s8 * jnp.exp(m8 - m), axis=0, keepdims=True)
        stats[0, r, half, q, 2:3, :] = jnp.sum(t8, axis=0, keepdims=True)
        ocopy(ts, q, slot).start()
        return 0

    lax.fori_loop(0, 16, step, 0)
    for copy in stat_copies(3):
        copy.start()
    for d in (1, 2, 3):
        narrive(nz, "z", zi, d).wait_recv()
    total = (nz[0] + nz[1] + nz[2] + nz[3])[0:1, 0:1]
    for d in range(4):
        for cross in range(2):
            if d or cross:
                for r in range(4):
                    scopy(r, d, cross).wait_recv()
    loss = jnp.zeros((1, TB), F32)
    for r in range(4):
        for half in range(2):
            for q in range(2):
                lanes = slice(q * TB, q * TB + TB)
                ms = [stats[i, r, half, q, 0:1, :] for i in range(8)]
                m = functools.reduce(jnp.maximum, ms)
                tot = sum(stats[i, r, half, q, 1:2, :] * jnp.exp(ms[i] - m) for i in range(8))
                tgt_logit = sum(stats[i, r, half, q, 2:3, :] for i in range(8))
                lse = m + jnp.log(tot)
                mask = ints[r, half, q, 2:3, :].astype(F32)
                row_ref[2 * r + half, 0:1, lanes] = lse
                row_ref[2 * r + half, 1:2, lanes] = mask / total
                ids_ref[2 * r + half, 0:1, lanes] = ints[r, half, q, 0:1, :] - vstart
                ids_ref[2 * r + half, 1:2, lanes] = ints[r, half, q, 1:2, :] - vstart
                if r == 0:
                    loss = loss + jnp.where(core == half, mask * (lse - tgt_logit), 0.0)
    aux_ref[...] = jnp.zeros_like(aux_ref)
    aux_ref[0:1, :] = jnp.broadcast_to(jnp.sum(loss, axis=1, keepdims=True), (1, 128))
    aux_ref[1:2, :] = jnp.broadcast_to(total, (1, 128))
    for copy in own + onward:
        copy.wait_send()
    for r in (1, 2, 3):
        for q in range(2):
            pcopy(r, q).wait_send()
    for d in (1, 2, 3):
        icopy(d).wait_send()
        ncopy(ny, "y", yi, d).wait_send()
        ncopy(nz, "z", zi, d).wait_send()
    for r in range(4):
        for copy in stat_copies(r):
            copy.wait_send()
    for slot in range(2):
        ocopy(0, 0, slot).wait()
    for ts in range(NS):
        for q in range(2):
            zcopy(ts, q).wait()
            fcopy(ts, q).wait()


def forward(h_t, ge_t, w, ints, et):
    dma = pltpu.SemaphoreType.DMA
    return pl.pallas_call(
        forward_kernel,
        out_shape=(
            jax.ShapeDtypeStruct((NS, VB, TS), F32),
            jax.ShapeDtypeStruct((NS, 2, D, TB), BF16),
            jax.ShapeDtypeStruct((NS, 2, D, TB), F32),
            jax.ShapeDtypeStruct((2, D, TB), F32),
            jax.ShapeDtypeStruct((NS, 8, TS), F32),
            jax.ShapeDtypeStruct((NS, 8, TS), I32),
            jax.ShapeDtypeStruct((8, 128), F32),
        ),
        in_specs=[VMEM, VMEM, VMEM, VMEM, ANY],
        out_specs=(ANY, ANY, ANY, VMEM, VMEM, VMEM, VMEM),
        scratch_shapes=[
            pltpu.VMEM((VB, D), BF16),
            pltpu.VMEM((2, VB, TB), F32),
            pltpu.VMEM((2, D, 512), BF16),
            pltpu.VMEM((NS, 2, D, TB), F32),
            pltpu.VMEM((NS, 2, D, TB), BF16),
            pltpu.VMEM((4, 2, 2, 8, TB), I32),
            pltpu.VMEM((8, 4, 2, 2, 8, TB), F32),
            pltpu.VMEM((4, 8, 128), F32),
            pltpu.VMEM((4, 8, 128), F32),
            dma((2,)), dma((2,)), dma((NS, 2)), dma((NS, 2)), dma((6,)), dma((4, 2)), dma((4, 2)), dma((4, 2)),
            dma((4,)), dma((4,)), dma((8, 4)), dma((8, 4)), dma((2, 4)), dma((2, 4)),
        ],
        compiler_params=pltpu.CompilerParams(vmem_limit_bytes=62 << 20, collective_id=0, has_side_effects=True),
    )(h_t, ge_t, w, ints, et)


def backward_kernel(et_ref, zt_ref, gt_ref, row_ref, ids_ref, logit_ref, dz_ref, de_ref, lbuf, et_s, lsem, esem):
    vstart = lax.axis_index("x") * VB
    iota = lax.broadcasted_iota(I32, (V2, TS), 0)

    def lcopy(vc, slot):
        return pltpu.make_async_copy(logit_ref.at[:, pl.ds(vc * V2, V2), :], lbuf.at[slot], lsem.at[slot])

    def ecopy(vc, slot):
        cols = pl.ds(pl.multiple_of(vstart + vc * V2, 128), V2)
        return pltpu.make_async_copy(et_ref.at[:, cols], et_s.at[slot], esem.at[slot])

    for slot in range(2):
        lcopy(slot, slot).start()
        ecopy(slot, slot).start()
    dz_ref[...] = jnp.zeros_like(dz_ref)

    def v_body(vc, _):
        slot = lax.rem(vc, 2)
        lcopy(vc, slot).wait()
        ecopy(vc, slot).wait()
        et = et_s[slot]
        base = vstart + vc * V2
        acc = jnp.zeros((D, V2), F32)
        for ts in range(NS):
            p = jnp.exp(lbuf[slot, ts] - row_ref[ts, 0:1, :])
            d = (jnp.where(iota == ids_ref[ts, 0:1, :] - vc * V2, p - 1.0, p) * row_ref[ts, 1:2, :]).astype(BF16)
            dz_ref[ts] += jnp.dot(et, d, preferred_element_type=F32)
            acc += lax.dot_general(zt_ref[ts], d, (((1,), (1,)), ((), ())), preferred_element_type=F32)
            o = jnp.where(iota == ids_ref[ts, 1:2, :] - vc * V2, 1.0, 0.0).astype(BF16)
            acc += lax.dot_general(gt_ref[ts].astype(BF16), o, (((1,), (1,)), ((), ())), preferred_element_type=F32)
        de_ref[vc] = acc
        nxt = jnp.minimum(vc + 2, N2 - 1)
        lcopy(nxt, slot).start()
        ecopy(nxt, slot).start()
        return 0

    lax.fori_loop(0, N2, v_body, 0)
    for slot in range(2):
        lcopy(0, slot).wait()
        ecopy(0, slot).wait()


def backward(et, zb, gb, row, ids, logit):
    return pl.pallas_call(
        backward_kernel,
        out_shape=(jax.ShapeDtypeStruct((NS, D, TS), F32), jax.ShapeDtypeStruct((N2, D, V2), F32)),
        in_specs=[ANY, VMEM, VMEM, VMEM, VMEM, ANY],
        out_specs=(VMEM, VMEM),
        scratch_shapes=[
            pltpu.VMEM((2, NS, V2, TS), F32),
            pltpu.VMEM((2, D, V2), BF16),
            pltpu.SemaphoreType.DMA((2,)),
            pltpu.SemaphoreType.DMA((2,)),
        ],
        compiler_params=pltpu.CompilerParams(vmem_limit_bytes=63 << 20),
    )(et, zb, gb, row, ids, logit)


def solution(mesh):
    mesh4 = Mesh(mesh.devices.reshape(2, 4, 4, 4), ("tp", "z", "y", "x"))

    def local_step(hidden, norm_w, embed, targets, loss_mask, token_ids, grad_embed):
        core, xi = lax.axis_index("tp"), lax.axis_index("x")
        h_t = hidden.reshape(TOK, D).T
        ge_t = grad_embed.reshape(TOK, D).T
        et = embed.T
        own = [a.reshape(2, 2, 1, TB) for a in (targets - core * VL, token_ids - core * VL, loss_mask)]
        ints = jnp.pad(jnp.concatenate(own, axis=2), ((0, 0), (0, 0), (0, 5), (0, 0)))
        logit, zb, uf, gf, row, ids, aux = forward(h_t, ge_t, norm_w.reshape(D, 1), ints, et)
        gg = lax.all_gather(gf, ("x", "tp"), axis=0)
        order = jnp.array([0, 0, 3, 3, 1, 1, 2, 2])
        half = jnp.array([0, 1] * 4)
        rel = lax.rem(xi + order, 4) * 2 + half
        gb = jnp.take(gg.transpose(0, 2, 1, 3).reshape(8, D, TS), rel, axis=0)
        zc = zb.transpose(0, 2, 1, 3).reshape(8, D, TS)
        loss_val = lax.psum(aux[0, 0], ("tp", "z", "y", "x")) / aux[1, 0]
        dz, de = backward(et, zc, gb, row, ids, logit)
        back = lax.rem(jnp.array([0, 1, 2, 3]) + 4 - xi, 4)
        slot = jnp.take(jnp.array([0, 2, 3, 1]), back)
        dz = jnp.take(dz.reshape(GX, 2, D, TS), slot, axis=0)
        dz = lax.psum_scatter(dz, "x", scatter_dimension=0, tiled=True)
        dz = lax.psum(dz, "tp").reshape(2, D, TS).transpose(1, 0, 2).reshape(D, TOK)
        de = de.transpose(1, 0, 2).reshape(D, 16, VB // 16).transpose(1, 0, 2)
        de = lax.psum_scatter(de, ("z", "y"), scatter_dimension=0, tiled=True)
        de = lax.all_to_all(de.reshape(64, 9, VB // 16), ("z", "y", "x"), 0, 0)
        de = de.reshape(16, GX, 9, VB // 16).transpose(2, 1, 0, 3).reshape(9, VL)
        rows = h_t.astype(F32)
        inv = lax.rsqrt(jnp.mean(rows * rows, axis=0, keepdims=True) + RMS_EPS)
        unit = rows * inv
        grad_gain = lax.psum(jnp.sum(dz * unit, axis=1), ("tp", "z", "y", "x")) * 0.5
        gu = dz * norm_w.astype(F32).reshape(D, 1)
        grad_hidden = inv * (gu - unit * jnp.mean(gu * unit, axis=0, keepdims=True))
        grad_hidden = grad_hidden.astype(BF16).T.reshape(1, TOK, D)
        return loss_val, grad_hidden, grad_gain, de.T

    dp = ("z", "y", "x")
    return jax.shard_map(
        local_step,
        mesh=mesh4,
        in_specs=(P(dp), P(), P("tp"), P(dp), P(dp), P(dp), P(dp)),
        out_specs=(P(), P(dp), P(), P("tp", dp)),
        check_vma=False,
    )
```

```python
import functools

import jax
import jax.numpy as jnp
from jax import lax
from jax.experimental import pallas as pl
from jax.experimental.pallas import tpu as pltpu
from jax.sharding import Mesh, PartitionSpec as P

RMS_EPS = 1e-6
F32, BF16, I32 = jnp.float32, jnp.bfloat16, jnp.int32
MESH = pl.DeviceIdType.MESH
D = 576
TOK = 1024
GX = 4
VL = 24576
VB = VL // GX
TS = 512
TB = 256
NS = GX * 2
V2 = 256
N2 = VB // V2
CH = 256
ROWS, LANE, OWN = 144, 128, 9
HROWS, HD, EC = ROWS // 2, D // 2, 512
VMEM = pl.BlockSpec(memory_space=pltpu.VMEM)
ANY = pl.BlockSpec(memory_space=pl.ANY)
V, DMA, SDS = pltpu.VMEM, pltpu.SemaphoreType.DMA, jax.ShapeDtypeStruct
SUB = 8
TOKENS = (NS, 2, D, TB)
SUMS = (SUB, 640)
GRID = [(dy, dx) for dy in range(4) for dx in range(4)]
FAR = GRID[1:]
GROUP = [(d, cross) for d in range(4) for cross in range(2) if d or cross]
PAIR, QUAD = range(2), range(4)
HOPS = QUAD[1:]
ROW0, ROW1, ROW2 = (slice(i, i + 1) for i in range(3))
NT = (((1,), (1,)), ((), ()))
FIRST, LATER = ((1, 0), (2, 1)), ((1, 1), (2, 0))
DELTA = (0, 3, 1, 2)
SLOT = [DELTA.index(d) for d in QUAD]


def span(i, n):
    return slice(i * n, i * n + n)


def sum4(buf):
    return (buf[0] + buf[1]) + (buf[2] + buf[3])


def two(n):
    return lax.rem(n, 2)


def four(n):
    return lax.rem(n, 4)


def side(i):
    return 1 + 2 * i


def remote(src, dst, send, recv, where):
    return pltpu.make_async_remote_copy(src_ref=src, dst_ref=dst, send_sem=send, recv_sem=recv, device_id=where, device_id_type=MESH)


def forward_kernel(
    h_ref, ge_ref, w_ref, ints_ref, et_ref,
    logit_ref, zb_out, uf_out, gf_out, row_ref, ids_ref, aux_ref,
    e_s, stage, ebuf, uf, zb, ints, stats, ny, nz,
    esem, osem, zsem, fsem, usend, urecv, psend, precv, isend, irecv, ssend, srecv, nsend, nrecv,
):
    core = lax.axis_index("tp")
    xi, yi, zi = lax.axis_index("x"), lax.axis_index("y"), lax.axis_index("z")
    other = 1 - core

    def at_x(d):
        return four(xi + d)

    right, left = at_x(1), at_x(3)
    vstart = xi * VB

    def ecopy(i, slot):
        cols = pl.ds(pl.multiple_of(vstart + i * EC, LANE), EC)
        return pltpu.make_async_copy(et_ref.at[:, cols], ebuf.at[slot], esem.at[slot])

    ecopy(0, 0).start()
    barrier = pltpu.get_barrier_semaphore()
    peers = [{"x": at_x(d)} for d in HOPS] + [{"x": at_x(d), "tp": other} for d in QUAD]
    peers += [{"y": four(yi + d)} for d in HOPS] + [{"z": four(zi + d)} for d in HOPS]
    for peer in peers:
        pl.semaphore_signal(barrier, inc=1, device_id=peer, device_id_type=MESH)

    ints[0] = ints_ref[...]
    weight = w_ref[...].astype(F32)
    for half in PAIR:
        for q in PAIR:
            lo = half * TS + q * TB
            rows = h_ref[:, lo:lo + TB].astype(F32)
            inv = lax.rsqrt(jnp.mean(rows * rows, axis=0, keepdims=True) + RMS_EPS)
            uf[half, q] = rows * inv
    for q in PAIR:
        lo = q * TB
        gf_out[q] = jnp.where(core == 0, ge_ref[:, lo:lo + TB].astype(F32), ge_ref[:, TS + lo:TS + lo + TB].astype(F32))
    pl.semaphore_wait(barrier, len(peers))

    def ucopy(src, q, dst, way, index):
        return remote(uf.at[2 * src + core, q], uf.at[2 * dst + core, q], usend.at[index], urecv.at[dst, q], {"x": way})

    def pcopy(r, q):
        return remote(uf.at[2 * r + core, q], uf.at[2 * r + core, q], psend.at[r, q], precv.at[r, q], {"tp": other})

    def parrive(r, q):
        return remote(uf.at[2 * r + core, q], uf.at[2 * r + other, q], psend.at[r, q], precv.at[r, q], {"tp": other})

    ways = (left, right)
    own = [ucopy(0, q, r, ways[r % 2], i) for i, (r, q) in enumerate(FIRST + LATER)]
    onward = [ucopy(r, q, 3, ways[r % 2], 4 + q) for r, q in FIRST]

    def icopy(d):
        return remote(ints.at[0], ints.at[SLOT[-d % 4]], isend.at[d], irecv.at[SLOT[-d % 4]], {"x": at_x(d)})

    for copy in own[:2]:
        copy.start()
    for d in HOPS:
        icopy(d).start()
    for copy in own[2:]:
        copy.start()

    def ebody(i, _):
        slot = two(i)

        @pl.when(i + 1 < VB // EC)
        def _():
            ecopy(i + 1, 1 - slot).start()

        ecopy(i, slot).wait()
        e_s[pl.ds(pl.multiple_of(i * EC, EC), EC), :] = ebuf[slot].T
        return 0

    lax.fori_loop(0, VB // EC, ebody, 0)

    def scopy(r, d, cross):
        index = 2 * d + cross
        where = {"x": at_x(d), "tp": other} if cross else {"x": at_x(d)}
        dst = SLOT[(DELTA[r] - d) % 4]
        return remote(stats.at[0, r], stats.at[index, dst], ssend.at[index, r], srecv.at[index, dst], where)

    def stat_copies(r):
        return [scopy(r, d, cross) for d, cross in GROUP]

    def ncopy(buf, axis, me, d):
        k = {"y": 0, "z": 1}[axis]
        return remote(buf.at[me], buf.at[me], nsend.at[k, d], nrecv.at[k, d], {axis: four(me + d)})

    def narrive(buf, axis, me, d):
        k = {"y": 0, "z": 1}[axis]
        return remote(buf.at[me], buf.at[four(me + 4 - d)], nsend.at[k, d], nrecv.at[k, d], {axis: four(me + d)})

    iota = lax.broadcasted_iota(I32, (8, TB), 0)

    def ocopy(ts, q, slot):
        return pltpu.make_async_copy(stage.at[slot], logit_ref.at[ts, :, pl.ds(pl.multiple_of(q * TB, TB), TB)], osem.at[slot])

    def zcopy(ts, q):
        return pltpu.make_async_copy(zb.at[ts, q], zb_out.at[ts, q], zsem.at[ts, q])

    def fcopy(ts, q):
        return pltpu.make_async_copy(uf.at[ts, q], uf_out.at[ts, q], fsem.at[ts, q])

    def step(s, _):
        j = four(s)
        r = jnp.where(s < 4, 0, jnp.where(s < 12, 1 + two(j), 3))
        q = jnp.where((s < 8) | (s >= 12), two(j), 1 - two(j))
        half = jnp.where(s < 4, j // 2, jnp.where(j < 2, core, other))
        ts = 2 * r + half

        @pl.when(s == 4)
        def _():
            for i, (r, q) in enumerate(FIRST):
                own[i].wait_recv()
                onward[i].start()
                pcopy(r, q).start()
            for d in HOPS:
                icopy(d).wait_recv()
            for copy in stat_copies(0):
                copy.start()

        @pl.when(s == 6)
        def _():
            for r, q in FIRST:
                parrive(r, q).wait_recv()

        @pl.when(s == 8)
        def _():
            for i, (r, q) in enumerate(LATER):
                own[2 + i].wait_recv()
                pcopy(r, q).start()
            count = jnp.sum(ints[:, :, :, 2, :].astype(F32))
            ny[yi] = jnp.full((8, LANE), count, F32)
            for d in HOPS:
                ncopy(ny, "y", yi, d).start()

        @pl.when(s == 10)
        def _():
            for r, q in LATER:
                parrive(r, q).wait_recv()
            for d in HOPS:
                narrive(ny, "y", yi, d).wait_recv()
            nz[zi] = sum4(ny)
            for d in HOPS:
                ncopy(nz, "z", zi, d).start()

        @pl.when(s == 12)
        def _():
            for i in PAIR:
                onward[i].wait_recv()
                pcopy(3, i).start()
            for copy in stat_copies(1) + stat_copies(2):
                copy.start()

        @pl.when(s == 14)
        def _():
            for i in PAIR:
                parrive(3, i).wait_recv()

        slot = two(s)

        @pl.when(s >= 2)
        def _():
            ocopy(ts, q, slot).wait()

        zt = (uf[ts, q] * weight).astype(BF16)
        zb[ts, q] = zt
        zcopy(ts, q).start()
        fcopy(ts, q).start()
        tgt = ints[r, half, q, ROW0, :] - vstart
        m8 = jnp.full((8, TB), -jnp.inf, F32)
        s8 = jnp.zeros((8, TB), F32)
        t8 = jnp.zeros((8, TB), F32)
        for vc in range(VB // CH):
            l = jnp.dot(e_s[vc * CH:(vc + 1) * CH, :], zt, preferred_element_type=F32)
            stage[slot, vc * CH:(vc + 1) * CH, :] = l
            mn = m8
            for i in range(CH // 8):
                mn = jnp.maximum(mn, l[span(i, 8)])
            s8 = s8 * jnp.exp(m8 - mn)
            m8 = mn
            for i in range(CH // 8):
                li = l[span(i, 8)]
                s8 = s8 + jnp.exp(li - mn)
                t8 = t8 + jnp.where(iota == tgt - (vc * CH + i * 8), li, 0.0)
        m = jnp.max(m8, axis=0, keepdims=True)
        stats[0, r, half, q, ROW0, :] = m
        stats[0, r, half, q, ROW1, :] = jnp.sum(s8 * jnp.exp(m8 - m), axis=0, keepdims=True)
        stats[0, r, half, q, ROW2, :] = jnp.sum(t8, axis=0, keepdims=True)
        ocopy(ts, q, slot).start()
        return 0

    lax.fori_loop(0, 16, step, 0)
    for copy in stat_copies(3):
        copy.start()
    for d in HOPS:
        narrive(nz, "z", zi, d).wait_recv()
    total = sum4(nz)[ROW0, ROW0]
    for r in QUAD:
        for copy in stat_copies(r):
            copy.wait_recv()
    loss = jnp.zeros((1, TB), F32)
    for r in QUAD:
        for half in PAIR:
            for q in PAIR:
                lanes = span(q, TB)
                ms = [stats[i, r, half, q, ROW0, :] for i in range(8)]
                m = functools.reduce(jnp.maximum, ms)
                tot = sum(stats[i, r, half, q, ROW1, :] * jnp.exp(ms[i] - m) for i in range(8))
                tgt_logit = sum(stats[i, r, half, q, ROW2, :] for i in range(8))
                lse = m + jnp.log(tot)
                mask = ints[r, half, q, ROW2, :].astype(F32)
                row_ref[2 * r + half, ROW0, lanes] = lse
                row_ref[2 * r + half, ROW1, lanes] = mask / total
                ids_ref[2 * r + half, ROW0, lanes] = ints[r, half, q, ROW0, :] - vstart
                ids_ref[2 * r + half, ROW1, lanes] = ints[r, half, q, ROW1, :] - vstart
                if r == 0:
                    loss = loss + jnp.where(core == half, mask * (lse - tgt_logit), 0.0)
    aux_ref[...] = jnp.zeros_like(aux_ref)
    aux_ref[ROW0, :] = jnp.broadcast_to(jnp.sum(loss, axis=1, keepdims=True), (1, LANE))
    aux_ref[ROW1, :] = jnp.broadcast_to(total, (1, LANE))
    for copy in own + onward:
        copy.wait_send()
    for r in HOPS:
        for q in PAIR:
            pcopy(r, q).wait_send()
    for d in HOPS:
        icopy(d).wait_send()
        ncopy(ny, "y", yi, d).wait_send()
        ncopy(nz, "z", zi, d).wait_send()
    for r in QUAD:
        for copy in stat_copies(r):
            copy.wait_send()
    for slot in PAIR:
        ocopy(0, 0, slot).wait()
    for ts in range(NS):
        for q in PAIR:
            zcopy(ts, q).wait()
            fcopy(ts, q).wait()


def forward(h_t, ge_t, w, ints, et):
    return pl.pallas_call(
        forward_kernel,
        out_shape=(
            SDS((NS, VB, TS), F32),
            SDS(TOKENS, BF16),
            SDS(TOKENS, F32),
            SDS(TOKENS[1:], F32),
            SDS((NS, SUB, TS), F32),
            SDS((NS, SUB, TS), I32),
            SDS((SUB, LANE), F32),
        ),
        in_specs=[VMEM] * 4 + [ANY],
        out_specs=(ANY,) * 3 + (VMEM,) * 4,
        scratch_shapes=[
            V((VB, D), BF16),
            V((2, VB, TB), F32),
            V((2, D, EC), BF16),
            V(TOKENS, F32),
            V(TOKENS, BF16),
            V((GX, 2, 2, SUB, TB), I32),
            V((NS, GX, 2, 2, SUB, TB), F32),
            *[V((GX, SUB, LANE), F32)] * 2,
            *[DMA((2,))] * 2, *[DMA((NS, 2))] * 2, DMA((NS,)), *[DMA((GX, 2))] * 3,
            *[DMA((GX,))] * 2, *[DMA((NS, GX))] * 2, *[DMA((2, GX))] * 2,
        ],
        compiler_params=pltpu.CompilerParams(vmem_limit_bytes=62 << 20, collective_id=0, has_side_effects=True),
    )(h_t, ge_t, w, ints, et)


NP = 6
NA = 16


def backward_kernel(
    et_ref, zb_ref, row_ref, ids_ref, logit_ref, gf_ref, uf_ref, ge_ref, h_ref, w_ref, aux_ref,
    de_out, dh_out, sum_out, gall,
    gb, dz, de, lbuf, et_s, gst, ra1, ra2, rb1, rb2, fin, sb, rv, dzp, rc1, rc2, hbuf, st, sx, sy, sz,
    lsem, esem, gsem, gown, hsem, gsend, grecv, gpsend, gprecv,
    a1s, a1r, a2s, a2r, b1s, b1r, b2s, b2r, ass, asr, dps, dpr, c1s, c1r, c2s, c2r, hs, hr, sts, str_, sas, sar,
):
    core = lax.axis_index("tp")
    xi, yi, zi = lax.axis_index("x"), lax.axis_index("y"), lax.axis_index("z")
    other = 1 - core
    me = {"x": xi, "y": yi, "z": zi}

    def at(axis, d):
        return four(me[axis] + d)

    right, left = at("x", 1), at("x", 3)
    vstart = xi * VB
    iota = lax.broadcasted_iota(I32, (V2, TS), 0)

    def lcopy(vc, slot):
        return pltpu.make_async_copy(logit_ref.at[:, pl.ds(pl.multiple_of(vc * V2, V2), V2), :], lbuf.at[slot], lsem.at[slot])

    def ecopy(vc, slot):
        cols = pl.ds(pl.multiple_of(vstart + vc * V2, LANE), V2)
        return pltpu.make_async_copy(et_ref.at[:, cols], et_s.at[slot], esem.at[slot])

    for slot in PAIR:
        lcopy(slot, slot).start()
        ecopy(slot, slot).start()
    barrier = pltpu.get_barrier_semaphore()
    peers = [{"y": at("y", dy), "x": at("x", dx)} for dy, dx in FAR]
    peers += [{"z": at("z", d)} for d in HOPS] + [{"tp": other}]
    for peer in peers:
        pl.semaphore_signal(barrier, inc=1, device_id=peer, device_id_type=MESH)
    pl.semaphore_wait(barrier, len(peers))

    def gcopy(q, dst, way, index):
        return remote(gf_ref.at[q], gall.at[2 * dst + core, q], gsend.at[index], grecv.at[dst, q], {"x": way})

    def gonward(src, q, way, index):
        return remote(gall.at[2 * src + core, q], gall.at[6 + core, q], gsend.at[index], grecv.at[3, q], {"x": way})

    def gpcopy(r, q):
        return remote(gall.at[2 * r + core, q], gall.at[2 * r + core, q], gpsend.at[r, q], gprecv.at[r, q], {"tp": other})

    def gparrive(r, q):
        return remote(gall.at[2 * r + core, q], gall.at[2 * r + other, q], gpsend.at[r, q], gprecv.at[r, q], {"tp": other})

    ways = (left, right)
    gown_copies = [gcopy(q, r, ways[r % 2], i) for i, (r, q) in enumerate(FIRST + LATER)]
    gonward_copies = [gonward(r, q, ways[r % 2], 4 + q) for r, q in FIRST]
    for copy in gown_copies:
        copy.start()

    def own_ge(half, q):
        return pltpu.make_async_copy(ge_ref.at[:, pl.ds(half * TS + q * TB, TB)], gb.at[half, q], gown.at[half, q])

    for half in PAIR:
        for q in PAIR:
            own_ge(half, q).start()
    hcopy = pltpu.make_async_copy(h_ref.at[:, pl.ds(pl.multiple_of(core * TS, TS), TS)], hbuf, hsem)
    hcopy.start()

    def piece(p):
        third = p >= 8
        hi = two(p // 2)
        r = jnp.where(third, 3, 1 + hi)
        q = jnp.where(third, hi, jnp.where(p < 4, hi, 1 - hi))
        return 2 * r + two(p), q

    def stage_in(p):
        ts, q = piece(p)
        return pltpu.make_async_copy(gall.at[ts, q], gst.at[two(p)], gsem.at[two(p)])

    def convert(p):
        ts, q = piece(p)
        stage_in(p).wait()
        gb[ts, q] = gst[two(p)].astype(BF16)

    dz[...] = jnp.zeros_like(dz)

    def de_index(u, zblk, qtr):
        return jnp.where(two(u) == 0, zblk * 4 + qtr, qtr * 4 + zblk)

    def logits_step(vc):
        slot = two(vc)
        lcopy(vc, slot).wait()
        ecopy(vc, slot).wait()
        et = et_s[slot]
        base = vc * V2
        acc = None
        for ts in range(NS):
            r, half = ts // 2, ts % 2
            p = jnp.exp(lbuf[slot, ts] - row_ref[ts, ROW0, :])
            d = (jnp.where(iota == ids_ref[ts, ROW0, :] - base, p - 1.0, p) * row_ref[ts, ROW1, :]).astype(BF16)
            dz[half, r] += jnp.dot(et, d, preferred_element_type=F32)
            for q in PAIR:
                a = lax.dot_general(zb_ref[ts, q], d[:, span(q, TB)], NT, preferred_element_type=F32)
                acc = a if acc is None else acc + a
        u = vc // 2
        for zblk in QUAD:
            for ql in PAIR:
                de[u, de_index(u, zblk, slot * 2 + ql)] = acc[span(zblk, ROWS), span(ql, LANE)]
        nxt = jnp.minimum(vc + 2, N2 - 1)
        lcopy(nxt, slot).start()
        ecopy(nxt, slot).start()

    def lookup_step(vc):
        base = vc * V2
        acc = None
        for ts in range(NS):
            o = jnp.where(iota == ids_ref[ts, ROW1, :] - base, 1.0, 0.0).astype(BF16)
            for q in PAIR:
                a = lax.dot_general(gb[ts, q], o[:, span(q, TB)], NT, preferred_element_type=F32)
                acc = a if acc is None else acc + a
        u = vc // 2
        for zblk in QUAD:
            for ql in PAIR:
                de[u, de_index(u, zblk, two(vc) * 2 + ql)] += acc[span(zblk, ROWS), span(ql, LANE)]

    AXES = ("zy", "yz")

    def hop(axis, i):
        return {axis: at(axis, side(i))}

    def a1(p, c):
        a, _ = AXES[c]
        k, op = two(p), at(a, 2) * 4
        return [remote(de.at[2 * p + c, pl.ds(op + 2 * i, 2)], ra1.at[c, k, i], a1s.at[c, k, i], a1r.at[c, k, i], hop(a, i)) for i in PAIR]

    def a2(p, c):
        a, _ = AXES[c]
        k = two(p)
        return [remote(de.at[2 * p + c, pl.ds(at(a, side(i)) * 4, 4)], ra2.at[c, k, i], a2s.at[c, k, i], a2r.at[c, k, i], hop(a, i)) for i in PAIR]

    def b1(p, c):
        a, b = AXES[c]
        k, i2 = two(p), me[a] * 4 + at(b, 2)
        return [remote(de.at[2 * p + c, i2, pl.ds(HROWS * i, HROWS)], rb1.at[c, k, i], b1s.at[c, k, i], b1r.at[c, k, i], hop(b, i)) for i in PAIR]

    def b2(p, c):
        a, b = AXES[c]
        k = two(p)
        return [remote(de.at[2 * p + c, me[a] * 4 + at(b, side(i))], rb2.at[c, k, i], b2s.at[c, k, i], b2r.at[c, k, i], hop(b, i)) for i in PAIR]

    def start(copies):
        for copy in copies:
            copy.start()

    def wait(copies):
        for copy in copies:
            copy.wait()

    def do_a1(p):
        for c in PAIR:
            start(a1(p, c))

    def do_a2(p):
        k = two(p)
        for c in PAIR:
            a, _ = AXES[c]
            wait(a1(p, c))
            for i in PAIR:
                for j in PAIR:
                    de[2 * p + c, at(a, side(i)) * 4 + 2 * i + j] += ra1[c, k, i, j]
            start(a2(p, c))

    def do_b1(p):
        k = two(p)
        for c in PAIR:
            a, _ = AXES[c]
            wait(a2(p, c))
            for j in QUAD:
                de[2 * p + c, me[a] * 4 + j] += ra2[c, k, 0, j] + ra2[c, k, 1, j]
            start(b1(p, c))

    def do_b2(p):
        k = two(p)
        for c in PAIR:
            a, b = AXES[c]
            wait(b1(p, c))
            for i in PAIR:
                de[2 * p + c, me[a] * 4 + at(b, side(i)), span(i, HROWS)] += rb1[c, k, i]
            start(b2(p, c))

    def do_f(p):
        k = two(p)
        for c in PAIR:
            a, b = AXES[c]
            wait(b2(p, c))
            fin[2 * p + c] = de[2 * p + c, me[a] * 4 + me[b]] + rb2[c, k, 0] + rb2[c, k, 1]

    def col(b, dy, dx):
        dst = at("y", dy) * 4 + at("x", dx)
        return remote(sb.at[b, dst], rv.at[b, yi * 4 + xi], ass.at[b, dy * 4 + dx], asr.at[b, dy * 4 + dx], {"y": at("y", dy), "x": at("x", dx)})

    def col_arrive(b, dy, dx):
        src = at("y", 4 - dy) * 4 + at("x", 4 - dx)
        return remote(sb.at[b, src], rv.at[b, src], ass.at[b, dy * 4 + dx], asr.at[b, dy * 4 + dx], {"y": at("y", dy), "x": at("x", dx)})

    def do_cols(b):
        for s in range(16):
            for k in range(6):
                sb[b, s, span(k, OWN), :] = fin[6 * b + k, span(s, OWN), :]
        for dy, dx in FAR:
            col(b, dy, dx).start()
        rv[b, yi * 4 + xi] = sb[b, yi * 4 + xi]

    def do_assemble(b):
        for dy, dx in FAR:
            col_arrive(b, dy, dx).wait_recv()
        for s in range(16):
            for k in range(6):
                lane = (s % 4) * VB + (6 * b + k) * EC + (s // 4) * LANE
                de_out[:, lane:lane + LANE] = rv[b, s, span(k, OWN), :]

    def phase_a(vc, _):
        @pl.when(vc == 6)
        def _():
            for i, (r, q) in enumerate(FIRST):
                gown_copies[i].wait_recv()
                gonward_copies[i].start()
                gpcopy(r, q).start()

        @pl.when(vc == 7)
        def _():
            for r, q in FIRST:
                gparrive(r, q).wait_recv()

        @pl.when(vc == 10)
        def _():
            for i, (r, q) in enumerate(LATER):
                gown_copies[2 + i].wait_recv()
                gpcopy(r, q).start()

        @pl.when(vc == 11)
        def _():
            for r, q in LATER:
                gparrive(r, q).wait_recv()

        @pl.when(vc >= 8)
        def _():
            convert(vc - 8)

        @pl.when((vc >= 7) & (vc < 15))
        def _():
            stage_in(vc - 7).start()

        logits_step(vc)
        return 0

    lax.fori_loop(0, NA, phase_a, 0)
    for i in PAIR:
        gonward_copies[i].wait_recv()
        gpcopy(3, i).start()
    for i in PAIR:
        gparrive(3, i).wait_recv()
    for half in PAIR:
        for q in PAIR:
            own_ge(half, q).wait()
    stage_in(8).start()
    for p in range(8, 12):
        if p < 11:
            stage_in(p + 1).start()
        convert(p)

    def phase_c(p, _):
        def lookups(i, _):
            lookup_step(4 * p + i)
            return 0

        lax.fori_loop(0, 4, lookups, 0)
        do_a1(p)

        @pl.when(p >= 2)
        def _():
            do_b2(p - 2)

        def more(i, _):
            logits_step(NA + 2 * p + i)
            return 0

        lax.fori_loop(0, 2, more, 0)
        do_a2(p)

        @pl.when(p >= 1)
        def _():
            do_b1(p - 1)

        @pl.when(p >= 2)
        def _():
            do_f(p - 2)

        return 0

    lax.fori_loop(0, 4, phase_c, 0)
    for slot in PAIR:
        lcopy(N2 - 1, slot).wait()
        ecopy(N2 - 1, slot).wait()

    def dcopy(r):
        return remote(dz.at[other, r], dzp.at[r], dps.at[r], dpr.at[r], {"tp": other})

    for r in (3, 1, 2, 0):
        dcopy(r).start()

    def ucopy(i):
        return pltpu.make_async_copy(uf_ref.at[i // 2, i % 2], gst.at[i % 2], gsem.at[i % 2])

    ucopy(0).start()
    total = jnp.zeros((D, LANE), F32)
    for i in range(16):
        if i < 15:
            ucopy(i + 1).start()
        ucopy(i).wait()
        r, half, q = i // 4, (i // 2) % 2, i % 2
        for j in PAIR:
            lo = q * TB + LANE * j
            total = total + dz[half, r, :, lo:lo + LANE] * gst[i % 2, :, span(j, LANE)]
    dg = jnp.sum(total.T, axis=0, keepdims=True)

    def sum_start(buf, axis):
        k = {"x": 0, "y": 1, "z": 2}[axis]
        for d in HOPS:
            remote(buf.at[me[axis]], buf.at[me[axis]], sas.at[k, d], sar.at[k, d], {axis: at(axis, d)}).start()

    def sum_wait(buf, axis):
        k = {"x": 0, "y": 1, "z": 2}[axis]
        for d in HOPS:
            remote(buf.at[me[axis]], buf.at[at(axis, 4 - d)], sas.at[k, d], sar.at[k, d], {axis: at(axis, d)}).wait()
        return sum4(buf)

    st[core] = jnp.zeros((8, 640), F32)
    st[core, 0:1, 0:D] = dg
    st[core, 1:2, 0:LANE] = aux_ref[ROW0, :]
    pair_copy = remote(st.at[core], st.at[core], sts, str_, {"tp": other})
    pair_arrive = remote(st.at[core], st.at[other], sts, str_, {"tp": other})
    def dz_add(r):
        dcopy(r).wait_recv()
        dz[core, r] += dzp[r]

    def c1(i):
        return remote(dz.at[core, 3, pl.ds(HD * i, HD)], rc1.at[i], c1s.at[i], c1r.at[i], hop("x", i))

    def c2(i):
        return remote(dz.at[core, 2 - i], rc2.at[i], c2s.at[i], c2r.at[i], hop("x", i))

    dz_add(3)
    for i in PAIR:
        c1(i).start()
    pair_copy.start()

    def lookups4(i, _):
        lookup_step(16 + i)
        return 0

    lax.fori_loop(0, 4, lookups4, 0)
    do_a1(4)
    do_b2(2)
    pair_arrive.wait()
    sx[xi] = st[0] + st[1]
    sum_start(sx, "x")
    dz_add(1)
    dz_add(2)
    do_b1(3)
    do_f(2)
    do_cols(0)

    def lookups5(i, _):
        lookup_step(20 + i)
        return 0

    lax.fori_loop(0, 4, lookups5, 0)
    do_a1(5)
    do_a2(4)
    do_b2(3)
    sy[yi] = sum_wait(sx, "x")
    sum_start(sy, "y")
    for i in PAIR:
        c1(i).wait()
        dz[core, 2 - i, span(i, HD)] += rc1[i]
        c2(i).start()
    dz_add(0)
    do_a2(5)
    sz[zi] = sum_wait(sy, "y")
    sum_start(sz, "z")
    do_f(3)
    do_b1(4)
    do_assemble(0)
    do_b2(4)
    do_b1(5)
    do_f(4)
    do_b2(5)
    sum_out[...] = sum_wait(sz, "z")
    do_f(5)
    do_cols(1)

    hcopy.wait()
    rows = hbuf[...].astype(F32)
    inv = lax.rsqrt(jnp.mean(rows * rows, axis=0, keepdims=True) + RMS_EPS)
    unit = rows * inv
    for i in PAIR:
        c2(i).wait()
    gu = (dz[core, 0] + rc2[0] + rc2[1]) * w_ref[...].astype(F32)
    dz[core, 3] = inv * (gu - unit * jnp.mean(gu * unit, axis=0, keepdims=True))
    half_copy = remote(dz.at[core, 3], dzp.at[3], hs, hr, {"tp": other})
    half_copy.start()
    do_assemble(1)
    half_copy.wait()
    for half in PAIR:
        dh_out[:, span(half, TS)] = jnp.where(core == half, dz[core, 3], dzp[3]).astype(BF16)

    for copy in gown_copies + gonward_copies:
        copy.wait_send()
    for r in HOPS:
        for q in PAIR:
            gpcopy(r, q).wait_send()
    for r in QUAD:
        dcopy(r).wait_send()
    for b in PAIR:
        for dy, dx in FAR:
            col(b, dy, dx).wait_send()


def backward(et, zb, row, ids, logit, gf, uf, ge_t, h_t, w, aux):
    return pl.pallas_call(
        backward_kernel,
        out_shape=(SDS((OWN, VL), F32), SDS((D, TOK), BF16), SDS(SUMS, F32), SDS(TOKENS, F32)),
        in_specs=[ANY] + [VMEM] * 3 + [ANY] * 5 + [VMEM] * 2,
        out_specs=(VMEM,) * 3 + (ANY,),
        scratch_shapes=[
            V(TOKENS, BF16),
            V((2, GX, D, TS), F32),
            V((2 * NP, 16, ROWS, LANE), F32),
            V((2, NS, V2, TS), F32),
            V((2, D, V2), BF16),
            V((2, D, TB), F32),
            V((2, 2, 2, 2, ROWS, LANE), F32),
            V((2, 2, 2, GX, ROWS, LANE), F32),
            V((2, 2, 2, HROWS, LANE), F32),
            V((2, 2, 2, ROWS, LANE), F32),
            V((2 * NP, ROWS, LANE), F32),
            *[V((2, 16, 56, LANE), F32)] * 2,
            V((GX, D, TS), F32),
            V((2, HD, TS), F32),
            V((2, D, TS), F32),
            V((D, TS), BF16),
            V((2, *SUMS), F32), *[V((GX, *SUMS), F32)] * 3,
            *[DMA((2,))] * 3, DMA((2, 2)), DMA(()), DMA((NS,)), *[DMA((GX, 2))] * 3,
            *[DMA((2, 2, 2))] * 8,
            *[DMA((2, 16))] * 2, *[DMA((GX,))] * 2, *[DMA((2,))] * 4, *[DMA(())] * 4, *[DMA((3, GX))] * 2,
        ],
        compiler_params=pltpu.CompilerParams(vmem_limit_bytes=67043328, collective_id=1, has_side_effects=True),
    )(et, zb, row, ids, logit, gf, uf, ge_t, h_t, w, aux)


def solution(mesh):
    mesh4 = Mesh(mesh.devices.reshape(2, 4, 4, 4), ("tp", "z", "y", "x"))

    def local_step(hidden, norm_w, embed, targets, loss_mask, token_ids, grad_embed):
        core = lax.axis_index("tp")
        h_t = hidden.reshape(TOK, D).T
        ge_t = grad_embed.reshape(TOK, D).T
        et = embed.T
        w = norm_w.reshape(D, 1)
        base = core * VL
        own = [a.reshape(2, 2, 1, TB) for a in (targets - base, token_ids - base, loss_mask)]
        ints = jnp.concatenate(own + own[:1] * 5, axis=2)
        logit, zb, uf, gf, row, ids, aux = forward(h_t, ge_t, w, ints, et)
        de, dh, sums, _ = backward(et, zb, row, ids, logit, gf, uf, ge_t, h_t, w, aux)
        loss_val = sums[1, 0] / aux[1, 0]
        return loss_val, dh.T.reshape(1, TOK, D), sums[0, :D], de.T

    dp = ("z", "y", "x")
    return jax.shard_map(
        local_step,
        mesh=mesh4,
        in_specs=(P(dp), P(), P("tp"), P(dp), P(dp), P(dp), P(dp)),
        out_specs=(P(), P(dp), P(), P("tp", dp)),
        check_vma=False,
    )
```

```python
import functools

import jax
import jax.numpy as jnp
from jax import lax
from jax.experimental import pallas as pl
from jax.experimental.pallas import tpu as pltpu
from jax.sharding import Mesh, PartitionSpec as P

RMS_EPS = 1e-6
F32, BF16, I32 = jnp.float32, jnp.bfloat16, jnp.int32
MESH = pl.DeviceIdType.MESH
D = 576
TOK = 1024
GX = 4
VL = 24576
VB = VL // GX
TS = 512
TB = 256
NS = GX * 2
V2 = 256
N2 = VB // V2
CH = 256
ROWS, LANE, OWN = 144, 128, 9
HROWS, HD, EC = ROWS // 2, D // 2, 512
VMEM = pl.BlockSpec(memory_space=pltpu.VMEM)
ANY = pl.BlockSpec(memory_space=pl.ANY)
V, DMA, SDS = pltpu.VMEM, pltpu.SemaphoreType.DMA, jax.ShapeDtypeStruct
SUB = 8
TOKENS = (NS, 2, D, TB)
SUMS = (SUB, 640)
GRID = [(dy, dx) for dy in range(4) for dx in range(4)]
FAR = GRID[1:]
GROUP = [(d, cross) for d in range(4) for cross in range(2) if d or cross]
PAIR, QUAD = range(2), range(4)
HOPS = QUAD[1:]
ROW0, ROW1, ROW2 = (slice(i, i + 1) for i in range(3))
NT = (((1,), (1,)), ((), ()))
FIRST, LATER = ((1, 0), (2, 1)), ((1, 1), (2, 0))
DELTA = (0, 3, 1, 2)
SLOT = [DELTA.index(d) for d in QUAD]


def span(i, n):
    return slice(i * n, i * n + n)


def sum4(buf):
    return (buf[0] + buf[1]) + (buf[2] + buf[3])


def two(n):
    return lax.rem(n, 2)


def four(n):
    return lax.rem(n, 4)


def side(i):
    return 1 + 2 * i


def remote(src, dst, send, recv, where):
    return pltpu.make_async_remote_copy(src_ref=src, dst_ref=dst, send_sem=send, recv_sem=recv, device_id=where, device_id_type=MESH)


NP = 6
NA = 9
AXES = ("zy", "yz")


def kernel(
    h_ref, ge_ref, w_ref, ints_ref, et_ref,
    de_out, dh_out, sum_out, logit_ref, uf_out, gall,
    uf, zb, gb, gst, ints, stats, hits, ny, nz, row, ids, aux,
    ra1, ra2, rb1, rb2, sb, rv, st, sx, sy, sz,
    etsem, osem, lsem, esem, gsem, gown, zsem, fsem,
    usend, urecv, psend, precv, isend, irecv, ssend, srecv, nsend, nrecv,
    gsend, grecv, gpsend, gprecv, a1s, a1r, a2s, a2r, b1s, b1r, b2s, b2r,
    ass, asr, dps, dpr, c1s, c1r, c2s, c2r, hs, hr, sts, str_, sas, sar,
):
    core = lax.axis_index("tp")
    me = {axis: lax.axis_index(axis) for axis in "xyz"}
    xi, yi, zi = (me[axis] for axis in "xyz")
    other = 1 - core
    vstart = xi * VB

    def at(axis, d):
        return four(me[axis] + d)

    def hop(axis, i):
        return {axis: at(axis, side(i))}

    barrier = pltpu.get_barrier_semaphore()
    peers = [{"y": at("y", dy), "x": at("x", dx)} for dy, dx in FAR]
    peers += [{"z": at("z", d)} for d in HOPS] + [{"x": at("x", d), "tp": other} for d in QUAD]
    for peer in peers:
        pl.semaphore_signal(barrier, inc=1, device_id=peer, device_id_type=MESH)

    def start(copies):
        for copy in copies:
            copy.start()

    def wait(copies):
        for copy in copies:
            copy.wait()

    def arrive(copies):
        for copy in copies:
            copy.wait_recv()

    def sent(copies):
        for copy in copies:
            copy.wait_send()

    right, left = at("x", 1), at("x", 3)
    ways = (left, right)

    def ucopy(src, q, dst, way, index):
        return remote(uf.at[2 * src + core, q], uf.at[2 * dst + core, q], usend.at[index], urecv.at[dst, q], {"x": way})

    def pcopy(r, q):
        return remote(uf.at[2 * r + core, q], uf.at[2 * r + core, q], psend.at[r, q], precv.at[r, q], {"tp": other})

    def parrive(r, q):
        return remote(uf.at[2 * r + core, q], uf.at[2 * r + other, q], psend.at[r, q], precv.at[r, q], {"tp": other})

    own = [ucopy(0, q, r, ways[r % 2], i) for i, (r, q) in enumerate(FIRST + LATER)]
    onward = [ucopy(r, q, 3, ways[r % 2], 4 + q) for r, q in FIRST]

    def gcopy(src, q, dst, way, index):
        return remote(gall.at[2 * src + core, q], gall.at[2 * dst + core, q], gsend.at[index], grecv.at[dst, q], {"x": way})

    def gpcopy(r, q):
        return remote(gall.at[2 * r + core, q], gall.at[2 * r + core, q], gpsend.at[r, q], gprecv.at[r, q], {"tp": other})

    def gparrive(r, q):
        return remote(gall.at[2 * r + core, q], gall.at[2 * r + other, q], gpsend.at[r, q], gprecv.at[r, q], {"tp": other})

    gmine = [gcopy(0, q, r, ways[r % 2], i) for i, (r, q) in enumerate(FIRST + LATER)]
    gonward = [gcopy(r, q, 3, ways[r % 2], 4 + q) for r, q in FIRST]

    def own_ge(half, q):
        return pltpu.make_async_copy(ge_ref.at[:, pl.ds(half * TS + q * TB, TB)], gb.at[half, q], gown.at[half, q])

    def out_dh(half, q):
        return pltpu.make_async_copy(gb.at[half, q], dh_out.at[:, pl.ds(half * TS + q * TB, TB)], gown.at[half, q])

    def keep_ge(q):
        return pltpu.make_async_copy(gst.at[q], gall.at[core, q], gsem.at[q])

    def icopy(d):
        return remote(ints.at[0], ints.at[SLOT[-d % 4]], isend.at[d], irecv.at[SLOT[-d % 4]], {"x": at("x", d)})

    def scopy(r, d, cross):
        index = 2 * d + cross
        where = {"x": at("x", d), "tp": other} if cross else {"x": at("x", d)}
        dst = SLOT[(DELTA[r] - d) % 4]
        return remote(stats.at[0, r], stats.at[index, dst], ssend.at[index, r], srecv.at[index, dst], where)

    def stat_copies(r):
        return [scopy(r, d, cross) for d, cross in GROUP]

    def gather_axis(buf, axis, sends, recvs):
        mine = me[axis]
        out = [remote(buf.at[mine], buf.at[mine], sends.at[d], recvs.at[d], {axis: at(axis, d)}) for d in HOPS]
        back = [remote(buf.at[mine], buf.at[at(axis, -d % 4)], sends.at[d], recvs.at[d], {axis: at(axis, d)}) for d in HOPS]
        return out, back

    ny_out, ny_in = gather_axis(ny, "y", nsend.at[0], nrecv.at[0])
    nz_out, nz_in = gather_axis(nz, "z", nsend.at[1], nrecv.at[1])

    def fcopy(ts, q):
        return pltpu.make_async_copy(uf.at[ts, q], uf_out.at[ts, q], fsem.at[ts, q])

    weight = w_ref[...].astype(F32)

    def forward(e_s, stage, etb):
        def etcopy(i):
            part = VB // 3
            cols = pl.ds(pl.multiple_of(vstart + i * part, LANE), part)
            return pltpu.make_async_copy(et_ref.at[:, cols], etb.at[:, pl.ds(i * part, part)], etsem.at[i])

        parts = [etcopy(i) for i in range(3)]
        start(parts)
        start([own_ge(half, q) for half in PAIR for q in PAIR])
        ints[0] = ints_ref[...]
        hits[...] = jnp.zeros_like(hits)
        for half in PAIR:
            for q in PAIR:
                rows = h_ref[:, pl.ds(half * TS + q * TB, TB)].astype(F32)
                inv = lax.rsqrt(jnp.mean(rows * rows, axis=0, keepdims=True) + RMS_EPS)
                uf[half, q] = rows * inv
        wait([own_ge(half, q) for half in PAIR for q in PAIR])
        for q in PAIR:
            gst[q] = gb[core, q].astype(F32)
        start([keep_ge(q) for q in PAIR])

        def ebody(i, _):
            lanes = pl.ds(pl.multiple_of(i * EC, EC), EC)
            e_s[lanes, :] = etb[:, lanes].T
            return 0

        for i, part in enumerate(parts):
            part.wait()
            lax.fori_loop(4 * i, 4 * i + 4, ebody, 0)
        wait([keep_ge(q) for q in PAIR])
        pl.semaphore_wait(barrier, len(peers))
        start(own[:2])
        start([icopy(d) for d in HOPS])
        start(own[2:])
        iota = lax.broadcasted_iota(I32, (SUB, TB), 0)

        def ocopy(ts, q, slot):
            return pltpu.make_async_copy(stage.at[slot], logit_ref.at[ts, :, pl.ds(pl.multiple_of(q * TB, TB), TB)], osem.at[slot])

        def zt_step(s, _):
            j = four(s)
            r = jnp.where(s < 4, 0, jnp.where(s < 12, 1 + two(j), 3))
            q = jnp.where((s < 8) | (s >= 12), two(j), 1 - two(j))
            half = jnp.where(s < 4, j // 2, jnp.where(j < 2, core, other))
            ts = 2 * r + half

            @pl.when(s == 4)
            def _():
                for i, (r, q) in enumerate(FIRST):
                    own[i].wait_recv()
                    onward[i].start()
                    pcopy(r, q).start()
                arrive([icopy(d) for d in HOPS])
                start(stat_copies(0))
                start(gmine[:2])

            @pl.when(s == 6)
            def _():
                arrive([parrive(r, q) for r, q in FIRST])

            @pl.when(s == 8)
            def _():
                for i, (r, q) in enumerate(LATER):
                    own[2 + i].wait_recv()
                    pcopy(r, q).start()
                count = jnp.sum(ints[:, :, :, 2, :].astype(F32))
                ny[yi] = jnp.full((SUB, LANE), count, F32)
                start(ny_out)

            @pl.when(s == 10)
            def _():
                arrive([parrive(r, q) for r, q in LATER])
                arrive(ny_in)
                nz[zi] = sum4(ny)
                start(nz_out)

            @pl.when(s == 12)
            def _():
                for i in PAIR:
                    onward[i].wait_recv()
                    pcopy(3, i).start()
                start(stat_copies(1) + stat_copies(2))

            @pl.when(s == 14)
            def _():
                arrive([parrive(3, i) for i in PAIR])

            slot = two(s)

            @pl.when(s >= 2)
            def _():
                ocopy(ts, q, slot).wait()

            zt = (uf[ts, q] * weight).astype(BF16)
            zb[ts, q] = zt
            fcopy(ts, q).start()
            tgt = ints[r, half, q, ROW0, :] - vstart
            m8 = jnp.full((SUB, TB), -jnp.inf, F32)
            s8 = jnp.zeros((SUB, TB), F32)
            t8 = jnp.zeros((SUB, TB), F32)
            for vc in range(VB // CH):
                l = jnp.dot(e_s[span(vc, CH), :], zt, preferred_element_type=F32)
                stage[slot, span(vc, CH), :] = l
                mn = m8
                for i in range(CH // SUB):
                    mn = jnp.maximum(mn, l[span(i, SUB)])
                s8 = s8 * jnp.exp(m8 - mn)
                m8 = mn
                for i in range(CH // SUB):
                    li = l[span(i, SUB)]
                    s8 = s8 + jnp.exp(li - mn)
                    t8 = t8 + jnp.where(iota == tgt - (vc * CH + i * SUB), li, 0.0)
            m = jnp.max(m8, axis=0, keepdims=True)
            at_row = 4 * half + 2 * q
            stats[0, r, pl.ds(at_row, 1), :] = m
            stats[0, r, pl.ds(at_row + 1, 1), :] = jnp.sum(s8 * jnp.exp(m8 - m), axis=0, keepdims=True)
            hits[...] += jnp.sum(t8, axis=0, keepdims=True) * ints[r, half, q, ROW2, :].astype(F32)
            ocopy(ts, q, slot).start()
            return 0

        lax.fori_loop(0, NS * 2, zt_step, 0)
        sent(own + onward + [pcopy(r, q) for r in HOPS for q in PAIR])
        wait([fcopy(ts, q) for ts in range(NS) for q in PAIR])
        start(stat_copies(3))
        start(gmine[2:])
        wait([ocopy(0, 0, slot) for slot in PAIR])

    pl.run_scoped(forward, V((VB, D), BF16), V((2, VB, TB), F32), V((D, VB), BF16))

    def backward(dz, de, lbuf, et_s):
        iota = lax.broadcasted_iota(I32, (V2, TS), 0)

        def near_load(vc):
            slot, rows = two(vc), pl.ds(pl.multiple_of(vc * V2, V2), V2)
            cols = pl.ds(pl.multiple_of(vstart + vc * V2, LANE), V2)
            return [
                pltpu.make_async_copy(logit_ref.at[pl.ds(0, NS - 2), rows, :], lbuf.at[slot, pl.ds(0, NS - 2)], lsem.at[slot, 0]),
                pltpu.make_async_copy(et_ref.at[:, cols], et_s.at[slot, :, pl.ds(0, V2)], esem.at[slot]),
            ]

        def far_load(u):
            slot, far = two(u), pl.ds(NS - 2, 2)
            cols = pl.ds(pl.multiple_of(vstart + u * EC, LANE), EC)
            return [
                pltpu.make_async_copy(logit_ref.at[far, pl.ds(pl.multiple_of(u * EC + k * V2, V2), V2), :], lbuf.at[slot, pl.ds(2 * k, 2)], lsem.at[slot, k])
                for k in PAIR
            ] + [pltpu.make_async_copy(et_ref.at[:, cols], et_s.at[slot], esem.at[slot])]

        for slot in PAIR:
            start(far_load(slot))
        dz[...] = jnp.zeros_like(dz)
        arrive(nz_in)
        total = sum4(nz)[ROW0, ROW0]
        for r in QUAD:
            arrive(stat_copies(r))
        loss = -hits[...]
        for r in QUAD:
            for half in PAIR:
                for q in PAIR:
                    lanes = span(q, TB)
                    top, low = (span(4 * half + 2 * q + i, 1) for i in PAIR)
                    ms = [stats[i, r, top, :] for i in range(NS)]
                    m = functools.reduce(jnp.maximum, ms)
                    tot = sum(stats[i, r, low, :] * jnp.exp(ms[i] - m) for i in range(NS))
                    lse = m + jnp.log(tot)
                    mask = ints[r, half, q, ROW2, :].astype(F32)
                    row[2 * r + half, ROW0, lanes] = lse
                    row[2 * r + half, ROW1, lanes] = mask / total
                    ids[2 * r + half, ROW0, lanes] = ints[r, half, q, ROW0, :] - vstart
                    ids[2 * r + half, ROW1, lanes] = ints[r, half, q, ROW1, :] - vstart
                    if r == 0:
                        loss = loss + jnp.where(core == half, mask * lse, 0.0)
        aux[0, ROW1, :] = jnp.broadcast_to(jnp.sum(loss, axis=1, keepdims=True), (1, TB))
        aux[1, ROW1, :] = jnp.broadcast_to(total, (1, TB))

        def piece(p):
            third = p >= 8
            hi = two(p // 2)
            r = jnp.where(third, 3, 1 + hi)
            q = jnp.where(third, hi, jnp.where(p < 4, hi, 1 - hi))
            return 2 * r + two(p), q

        def stage_in(p):
            ts, q = piece(p)
            return pltpu.make_async_copy(gall.at[ts, q], gst.at[two(p)], gsem.at[two(p)])

        def convert(p):
            ts, q = piece(p)
            stage_in(p).wait()
            gb[ts, q] = gst[two(p)].astype(BF16)

        def de_index(u, zblk, qtr):
            return jnp.where(two(u) == 0, zblk * 4 + qtr, qtr * 4 + zblk)

        def dlogits(tile, ts, base):
            p = jnp.exp(tile - row[ts, ROW0, :])
            return (jnp.where(iota == ids[ts, ROW0, :] - base, p - 1.0, p) * row[ts, ROW1, :]).astype(BF16)

        def products(et, ds, ts, accs):
            part = sum(jnp.dot(et[:, span(k, V2)], d, preferred_element_type=F32) for k, d in enumerate(ds))
            for q in PAIR:
                dz[ts % 2, ts // 2, q] += part[:, span(q, TB)]
                for k, d in enumerate(ds):
                    a = lax.dot_general(zb[ts, q], d[:, span(q, TB)], NT, preferred_element_type=F32)
                    accs[k] = a if accs[k] is None else accs[k] + a

        def far_step(u):
            slot, accs = two(u), [None, None]
            wait(far_load(u))
            et = et_s[slot]
            for half in PAIR:
                ts = NS - 2 + half
                products(et, [dlogits(lbuf[slot, 2 * k + half], ts, u * EC + k * V2) for k in PAIR], ts, accs)
            for zblk in QUAD:
                for qtr in QUAD:
                    de[u, de_index(u, zblk, qtr)] = accs[qtr // 2][span(zblk, ROWS), span(qtr % 2, LANE)]

            @pl.when(u + 2 < 2 * NP)
            def _():
                start(far_load(u + 2))

            @pl.when(u + 2 >= 2 * NP)
            def _():
                start(near_load(u + 2 - 2 * NP))

        def near_step(vc):
            slot, accs, u = two(vc), [None], vc // 2
            wait(near_load(vc))
            et = et_s[slot, :, span(0, V2)]
            for ts in range(NS - 2):
                products(et, [dlogits(lbuf[slot, ts], ts, vc * V2)], ts, accs)
            for zblk in QUAD:
                for ql in PAIR:
                    de[u, de_index(u, zblk, slot * 2 + ql)] += accs[0][span(zblk, ROWS), span(ql, LANE)]

            @pl.when(vc + 2 < N2)
            def _():
                start(near_load(vc + 2))

        def lookup_step(vc):
            base = vc * V2
            acc = None
            for ts in range(NS):
                o = jnp.where(iota == ids[ts, ROW1, :] - base, 1.0, 0.0).astype(BF16)
                for q in PAIR:
                    a = lax.dot_general(gb[ts, q], o[:, span(q, TB)], NT, preferred_element_type=F32)
                    acc = a if acc is None else acc + a
            u = vc // 2
            for zblk in QUAD:
                for ql in PAIR:
                    de[u, de_index(u, zblk, two(vc) * 2 + ql)] += acc[span(zblk, ROWS), span(ql, LANE)]

        def lookups(first):
            def one(i, _):
                lookup_step(first + i)
                return 0

            lax.fori_loop(0, 4, one, 0)

        def a1(p, c):
            a, _ = AXES[c]
            k, op = two(p), at(a, 2) * 4
            return [remote(de.at[2 * p + c, pl.ds(op + 2 * i, 2)], ra1.at[c, k, i], a1s.at[c, k, i], a1r.at[c, k, i], hop(a, i)) for i in PAIR]

        def a2(p, c):
            a, _ = AXES[c]
            k = two(p)
            return [remote(de.at[2 * p + c, pl.ds(at(a, side(i)) * 4, 4)], ra2.at[c, k, i], a2s.at[c, k, i], a2r.at[c, k, i], hop(a, i)) for i in PAIR]

        def b1(p, c):
            a, b = AXES[c]
            k, i2 = two(p), me[a] * 4 + at(b, 2)
            return [remote(de.at[2 * p + c, i2, pl.ds(HROWS * i, HROWS)], rb1.at[c, k, i], b1s.at[c, k, i], b1r.at[c, k, i], hop(b, i)) for i in PAIR]

        def b2(p, c):
            a, b = AXES[c]
            k = two(p)
            return [remote(de.at[2 * p + c, me[a] * 4 + at(b, side(i))], rb2.at[c, k, i], b2s.at[c, k, i], b2r.at[c, k, i], hop(b, i)) for i in PAIR]

        def do_a1(p):
            for c in PAIR:
                start(a1(p, c))

        def do_a2(p):
            k = two(p)
            for c in PAIR:
                a, _ = AXES[c]
                wait(a1(p, c))
                for i in PAIR:
                    for j in PAIR:
                        de[2 * p + c, at(a, side(i)) * 4 + 2 * i + j] += ra1[c, k, i, j]
                start(a2(p, c))

        def do_b1(p):
            k = two(p)
            for c in PAIR:
                a, _ = AXES[c]
                wait(a2(p, c))
                for j in QUAD:
                    de[2 * p + c, me[a] * 4 + j] += ra2[c, k, 0, j] + ra2[c, k, 1, j]
                start(b1(p, c))

        def do_b2(p):
            k = two(p)
            for c in PAIR:
                a, b = AXES[c]
                wait(b1(p, c))
                for i in PAIR:
                    de[2 * p + c, me[a] * 4 + at(b, side(i)), span(i, HROWS)] += rb1[c, k, i]
                start(b2(p, c))

        def do_f(p):
            k = two(p)
            for c in PAIR:
                a, b = AXES[c]
                wait(b2(p, c))
                de[2 * p + c, me[a] * 4 + me[b]] += rb2[c, k, 0] + rb2[c, k, 1]

        def col(b, dy, dx):
            dst = at("y", dy) * 4 + at("x", dx)
            return remote(sb.at[b, dst], rv.at[b, yi * 4 + xi], ass.at[b, dy * 4 + dx], asr.at[b, dy * 4 + dx], {"y": at("y", dy), "x": at("x", dx)})

        def col_arrive(b, dy, dx):
            src = at("y", -dy % 4) * 4 + at("x", -dx % 4)
            return remote(sb.at[b, src], rv.at[b, src], ass.at[b, dy * 4 + dx], asr.at[b, dy * 4 + dx], {"y": at("y", dy), "x": at("x", dx)})

        def do_cols(b):
            for k in range(NP):
                first, second = AXES[k % 2]
                mine = me[first] * 4 + me[second]
                for s in range(16):
                    sb[b, s, span(k, OWN), :] = de[NP * b + k, mine, span(s, OWN), :]
            start([col(b, dy, dx) for dy, dx in FAR])
            rv[b, yi * 4 + xi] = sb[b, yi * 4 + xi]

        def do_assemble(b):
            arrive([col_arrive(b, dy, dx) for dy, dx in FAR])
            for s in range(16):
                for k in range(NP):
                    lane = (s % 4) * VB + (NP * b + k) * EC + (s // 4) * LANE
                    de_out[:, pl.ds(lane, LANE)] = rv[b, s, span(k, OWN), :]

        def dcopy(r):
            return remote(dz.at[other, r], uf.at[r], dps.at[r], dpr.at[r], {"tp": other})

        def unit_in(r, q):
            return pltpu.make_async_copy(uf_out.at[2 * r + core, q], gst.at[q], gsem.at[q])

        def fetch(r):
            start([unit_in(r, q) for q in PAIR])

        def core_sum(r):
            dcopy(r).wait_recv()
            for q in PAIR:
                dz[core, r, q] += uf[r, q]

        def gain_sum(r, dg):
            wait([unit_in(r, q) for q in PAIR])
            for q in PAIR:
                for j in PAIR:
                    dg = dg + dz[core, r, q, :, span(j, LANE)] * gst[q, :, span(j, LANE)]
            return dg

        def c1(i, q):
            return remote(dz.at[core, 3, q, pl.ds(HD * i, HD)], uf.at[6, i, pl.ds(HD * q, HD)], c1s.at[i, q], c1r.at[i, q], hop("x", i))

        def c2(i):
            return remote(dz.at[core, 2 - i], uf.at[4 + i], c2s.at[i], c2r.at[i], hop("x", i))

        def far_unit(u, _):
            @pl.when(u == 2)
            def _():
                for i, (r, q) in enumerate(FIRST):
                    gmine[i].wait_recv()
                    gonward[i].start()
                    gpcopy(r, q).start()

            @pl.when(u == 4)
            def _():
                arrive([gparrive(r, q) for r, q in FIRST])
                stage_in(0).start()

            @pl.when((u >= 5) & (u < 9))
            def _():
                convert(u - 5)

            @pl.when((u >= 5) & (u < 8))
            def _():
                stage_in(u - 4).start()

            far_step(u)
            return 0

        lax.fori_loop(0, 2 * NP, far_unit, 0)
        dcopy(3).start()

        def near_chunk(vc, _):
            @pl.when(vc == 1)
            def _():
                for i, (r, q) in enumerate(LATER):
                    gmine[2 + i].wait_recv()
                    gpcopy(r, q).start()

            @pl.when(vc == 2)
            def _():
                arrive([gparrive(r, q) for r, q in LATER])
                stage_in(4).start()
                core_sum(3)
                start([c1(i, q) for i in PAIR for q in PAIR])

            @pl.when((vc >= 3) & (vc < 7))
            def _():
                convert(vc + 1)

            @pl.when((vc >= 3) & (vc < 6))
            def _():
                stage_in(vc + 2).start()

            near_step(vc)
            return 0

        lax.fori_loop(0, NA, near_chunk, 0)
        for i in PAIR:
            gonward[i].wait_recv()
            gpcopy(3, i).start()
        arrive([gparrive(3, i) for i in PAIR])
        stage_in(8).start()
        for p in range(8, 12):
            if p < 11:
                stage_in(p + 1).start()
            convert(p)

        def phase_c(p, _):
            @pl.when(p >= 1)
            def _():
                do_a2(p - 1)

            lookups(4 * p)

            @pl.when(p >= 2)
            def _():
                do_b2(p - 2)

            do_a1(p)

            def more(i, _):
                near_step(NA + 3 * p + i)
                return 0

            lax.fori_loop(0, 3, more, 0)

            @pl.when(p >= 2)
            def _():
                do_f(p - 2)

            @pl.when(p >= 1)
            def _():
                do_b1(p - 1)

            return 0

        lax.fori_loop(0, NP - 1, phase_c, 0)

        start([dcopy(r) for r in (1, 2, 0)])
        fetch(3)
        do_a2(4)
        do_cols(0)
        dg = gain_sum(3, jnp.zeros((D, LANE), F32))
        fetch(1)
        for i in (1, 0):
            core_sum(2 - i)
            dg = gain_sum(2 - i, dg)
            fetch(2 * i)
            for q in PAIR:
                c1(i, q).wait()
                dz[core, 2 - i, q, span(i, HD)] += uf[6, i, span(q, HD)]
            c2(i).start()
        lookups(20)
        do_b2(3)
        do_a1(5)
        core_sum(0)
        dg = gain_sum(0, dg)
        st[core] = jnp.zeros((SUB, 640), F32)
        st[core, ROW0, span(0, D)] = jnp.sum(dg.T, axis=0, keepdims=True)
        st[core, ROW1, span(0, TB)] = aux[0, ROW1, :]
        pair_copy = remote(st.at[core], st.at[core], sts, str_, {"tp": other})
        pair_arrive = remote(st.at[core], st.at[other], sts, str_, {"tp": other})
        pair_copy.start()
        do_b1(4)
        pair_arrive.wait()
        sz[zi] = st[0] + st[1]
        sums = [gather_axis(buf, axis, sas.at[k], sar.at[k]) for k, (buf, axis) in enumerate(((sz, "z"), (sy, "y"), (sx, "x")))]
        start(sums[0][0])
        do_a2(5)
        do_f(3)
        do_b2(4)
        wait(sums[0][1])
        sy[yi] = sum4(sz)
        start(sums[1][0])
        do_f(4)
        do_b1(5)
        wait(sums[1][1])
        sx[xi] = sum4(sy)
        start(sums[2][0])
        do_b2(5)
        do_f(5)
        do_cols(1)

        for q in PAIR:
            rows = h_ref[:, pl.ds(pl.multiple_of(core * TS + q * TB, TB), TB)].astype(F32)
            inv = lax.rsqrt(jnp.mean(rows * rows, axis=0, keepdims=True) + RMS_EPS)
            gst[q] = rows * inv
            aux[q, ROW0, :] = inv
        wait([c2(i) for i in PAIR])
        for q in PAIR:
            unit, inv = gst[q], aux[q, ROW0, :]
            gu = (dz[core, 0, q] + uf[4, q] + uf[5, q]) * weight
            dz[core, 3, q] = inv * (gu - unit * jnp.mean(gu * unit, axis=0, keepdims=True))
        half_copy = remote(dz.at[core, 3], uf.at[7], hs, hr, {"tp": other})
        half_copy.start()
        do_assemble(0)
        do_assemble(1)
        wait(sums[2][1])
        sum_out[...] = sum4(sx)
        sum_out[ROW1, span(0, TB)] = sum_out[ROW1, span(0, TB)] / aux[1, ROW1, :]
        half_copy.wait()
        for half in PAIR:
            for q in PAIR:
                gb[half, q] = jnp.where(core == half, dz[core, 3, q], uf[7, q]).astype(BF16)
                out_dh(half, q).start()
        wait([out_dh(half, q) for half in PAIR for q in PAIR])

        sent(gmine + gonward + [gpcopy(r, q) for r in HOPS for q in PAIR] + [dcopy(r) for r in QUAD])
        sent([col(b, dy, dx) for b in PAIR for dy, dx in FAR])
    pl.run_scoped(
        backward, V((2, GX, 2, D, TB), F32), V((2 * NP, 16, ROWS, LANE), F32), V((2, NS, V2, TS), F32), V((2, D, EC), BF16)
    )
    sent([icopy(d) for d in HOPS] + ny_out + nz_out)
    for r in QUAD:
        sent(stat_copies(r))


def call(h_t, ge_t, w, ints, et):
    links = [DMA((2, 2, 2))] * 8
    return pl.pallas_call(
        kernel,
        out_shape=(
            SDS((OWN, VL), F32), SDS((D, TOK), BF16), SDS(SUMS, F32),
            SDS((NS, VB, TS), F32), SDS(TOKENS, F32), SDS(TOKENS, F32),
        ),
        in_specs=[VMEM, ANY, VMEM, VMEM, ANY],
        out_specs=(VMEM, ANY, VMEM) + (ANY,) * 3,
        scratch_shapes=[
            V(TOKENS, F32),
            *[V(TOKENS, BF16)] * 2,
            V((2, D, TB), F32),
            V((GX, 2, 2, SUB, TB), I32),
            V((NS, GX, SUB, TB), F32), V((1, TB), F32),
            *[V((GX, SUB, LANE), F32)] * 2,
            V((NS, 2, TS), F32), V((NS, 2, TS), I32), V((2, SUB, TB), F32),
            V((2, 2, 2, 2, ROWS, LANE), F32),
            V((2, 2, 2, GX, ROWS, LANE), F32),
            V((2, 2, 2, HROWS, LANE), F32),
            V((2, 2, 2, ROWS, LANE), F32),
            *[V((2, 16, 56, LANE), F32)] * 2,
            V((2, *SUMS), F32), *[V((GX, *SUMS), F32)] * 3,
            DMA((3,)), DMA((2,)), DMA((2, 2)), *[DMA((2,))] * 2, DMA((2, 2)), *[DMA((NS, 2))] * 2,
            DMA((NS,)), *[DMA((GX, 2))] * 3, *[DMA((GX,))] * 2, *[DMA((NS, GX))] * 2, *[DMA((2, GX))] * 2,
            DMA((NS,)), *[DMA((GX, 2))] * 3, *links,
            *[DMA((2, 16))] * 2, *[DMA((GX,))] * 2, *[DMA((2, 2))] * 2, *[DMA((2,))] * 2, *[DMA(())] * 4, *[DMA((3, GX))] * 2,
        ],
        compiler_params=pltpu.CompilerParams(vmem_limit_bytes=67043328, collective_id=0, has_side_effects=True),
    )(h_t, ge_t, w, ints, et)


def solution(mesh):
    mesh4 = Mesh(mesh.devices.reshape(2, 4, 4, 4), ("tp", "z", "y", "x"))

    def local_step(hidden, norm_w, embed, targets, loss_mask, token_ids, grad_embed):
        base = lax.axis_index("tp") * VL
        h_t = hidden.reshape(TOK, D).T
        ge_t = grad_embed.reshape(TOK, D).T
        own = [a.reshape(2, 2, 1, TB) for a in (targets - base, token_ids - base, loss_mask)]
        ints = jnp.concatenate(own + own[:1] * 5, axis=2)
        de, dh, sums, *_ = call(h_t, ge_t, norm_w.reshape(D, 1), ints, embed.T)
        return sums[1, 0], dh.T.reshape(1, TOK, D), sums[0, :D], de.T

    dp = ("z", "y", "x")
    return jax.shard_map(
        local_step,
        mesh=mesh4,
        in_specs=(P(dp), P(), P("tp"), P(dp), P(dp), P(dp), P(dp)),
        out_specs=(P(), P(dp), P(), P("tp", dp)),
        check_vma=False,
    )
```

```python
import functools

import jax
import jax.numpy as jnp
from jax import lax
from jax.experimental import pallas as pl
from jax.experimental.pallas import tpu as pltpu
from jax.sharding import Mesh, PartitionSpec as P

RMS_EPS = 1e-6
F32, BF16, I32 = jnp.float32, jnp.bfloat16, jnp.int32
MESH = pl.DeviceIdType.MESH
D = 576
TOK = 1024
GX = 4
VL = 24576
VB = VL // GX
TS = 512
TB = 256
NS = GX * 2
V2 = 256
N2 = VB // V2
CH = 256
ROWS, LANE, OWN = 144, 128, 9
HROWS, HD, EC = ROWS // 2, D // 2, 512
VMEM = pl.BlockSpec(memory_space=pltpu.VMEM)
ANY = pl.BlockSpec(memory_space=pl.ANY)
V, DMA, SDS = pltpu.VMEM, pltpu.SemaphoreType.DMA, jax.ShapeDtypeStruct
SUB = 8
TOKENS = (NS, 2, D, TB)
SUMS = (2, 640)
GRID = [(dy, dx) for dy in range(4) for dx in range(4)]
FAR = GRID[1:]
GROUP = [(d, cross) for d in range(4) for cross in range(2) if d or cross]
PAIR, QUAD = range(2), range(4)
HOPS = QUAD[1:]
ROW0, ROW1, ROW2 = (slice(i, i + 1) for i in range(3))
NT = (((1,), (1,)), ((), ()))
FIRST, LATER = ((1, 0), (2, 1)), ((1, 1), (2, 0))
DELTA = (0, 3, 1, 2)
SLOT = [DELTA.index(d) for d in QUAD]


def span(i, n):
    return slice(i * n, i * n + n)


def sum4(buf):
    return (buf[0] + buf[1]) + (buf[2] + buf[3])


def two(n):
    return lax.rem(n, 2)


def four(n):
    return lax.rem(n, 4)


def side(i):
    return 1 + 2 * i


def remote(src, dst, send, recv, where):
    return pltpu.make_async_remote_copy(src_ref=src, dst_ref=dst, send_sem=send, recv_sem=recv, device_id=where, device_id_type=MESH)


NEARS, BATCHES = NS - 2, range(3)
NP = 6
NA = 4
AXES = ("zy", "yz")


def kernel(
    h_ref, ge_ref, w_ref, tgt_ref, mask_ref, tok_ref, et_ref,
    de_out, dh_out, sum_out, logit_ref, uf_out, gall,
    uf, zb, gb, gst, ints, stats, hits, ny, nz, row, ids, aux,
    gain, de_s, ra1, ra2, rb1, rb2, sb, rv, st, sx, sy, sz,
    desem, etsem, osem, lsem, esem, gsem, gown, zsem, fsem,
    usend, urecv, psend, precv, isend, irecv, ssend, srecv, nsend, nrecv,
    gsend, grecv, gpsend, gprecv, a1s, a1r, a2s, a2r, b1s, b1r, b2s, b2r,
    ass, asr, dps, dpr, c1s, c1r, c2s, c2r, hs, hr, sts, str_, sas, sar,
):
    core = lax.axis_index("tp")
    me = {axis: lax.axis_index(axis) for axis in "xyz"}
    xi, yi, zi = (me[axis] for axis in "xyz")
    other = 1 - core
    vstart = xi * VB

    def at(axis, d):
        return four(me[axis] + d)

    def hop(axis, i):
        return {axis: at(axis, side(i))}

    barrier = pltpu.get_barrier_semaphore()
    peers = [{"y": at("y", dy), "x": at("x", dx)} for dy, dx in FAR]
    peers += [{"z": at("z", d)} for d in HOPS] + [{"x": at("x", d), "tp": other} for d in QUAD]
    for peer in peers:
        pl.semaphore_signal(barrier, inc=1, device_id=peer, device_id_type=MESH)

    def start(copies):
        for copy in copies:
            copy.start()

    def wait(copies):
        for copy in copies:
            copy.wait()

    def arrive(copies):
        for copy in copies:
            copy.wait_recv()

    def sent(copies):
        for copy in copies:
            copy.wait_send()

    right, left = at("x", 1), at("x", 3)
    ways = (left, right)

    def ucopy(src, q, dst, way, index):
        return remote(uf.at[2 * src + core, q], uf.at[2 * dst + core, q], usend.at[index], urecv.at[dst, q], {"x": way})

    def pcopy(r, q):
        return remote(uf.at[2 * r + core, q], uf.at[2 * r + core, q], psend.at[r, q], precv.at[r, q], {"tp": other})

    def parrive(r, q):
        return remote(uf.at[2 * r + core, q], uf.at[2 * r + other, q], psend.at[r, q], precv.at[r, q], {"tp": other})

    own = [ucopy(0, q, r, ways[r % 2], i) for i, (r, q) in enumerate(FIRST + LATER)]
    onward = [ucopy(r, q, 3, ways[r % 2], 4 + q) for r, q in FIRST]

    def gcopy(src, q, dst, way, index):
        return remote(gall.at[2 * src + core, q], gall.at[2 * dst + core, q], gsend.at[index], grecv.at[dst, q], {"x": way})

    def gpcopy(r, q):
        return remote(gall.at[2 * r + core, q], gall.at[2 * r + core, q], gpsend.at[r, q], gprecv.at[r, q], {"tp": other})

    def gparrive(r, q):
        return remote(gall.at[2 * r + core, q], gall.at[2 * r + other, q], gpsend.at[r, q], gprecv.at[r, q], {"tp": other})

    gmine = [gcopy(0, q, r, ways[r % 2], i) for i, (r, q) in enumerate(FIRST + LATER)]
    gonward = [gcopy(r, q, 3, ways[r % 2], 4 + q) for r, q in FIRST]

    def own_ge(half, q):
        return pltpu.make_async_copy(ge_ref.at[:, pl.ds(half * TS + q * TB, TB)], gb.at[half, q], gown.at[half, q])

    def out_dh(half, q):
        return pltpu.make_async_copy(gb.at[half, q], dh_out.at[:, pl.ds(half * TS + q * TB, TB)], gown.at[half, q])

    def keep_ge(q):
        return pltpu.make_async_copy(gst.at[q], gall.at[core, q], gsem.at[q])

    def icopy(d):
        return remote(ints.at[0], ints.at[SLOT[-d % 4]], isend.at[d], irecv.at[SLOT[-d % 4]], {"x": at("x", d)})

    def scopy(r, d, cross):
        index = 2 * d + cross
        where = {"x": at("x", d), "tp": other} if cross else {"x": at("x", d)}
        dst = SLOT[(DELTA[r] - d) % 4]
        return remote(stats.at[0, r], stats.at[index, dst], ssend.at[index, r], srecv.at[index, dst], where)

    def stat_copies(r):
        return [scopy(r, d, cross) for d, cross in GROUP]

    def gather_axis(buf, axis, sends, recvs):
        mine = me[axis]
        out = [remote(buf.at[mine], buf.at[mine], sends.at[d], recvs.at[d], {axis: at(axis, d)}) for d in HOPS]
        back = [remote(buf.at[mine], buf.at[at(axis, -d % 4)], sends.at[d], recvs.at[d], {axis: at(axis, d)}) for d in HOPS]
        return out, back

    ny_out, ny_in = gather_axis(ny, "y", nsend.at[0], nrecv.at[0])
    nz_out, nz_in = gather_axis(nz, "z", nsend.at[1], nrecv.at[1])

    def fcopy(ts, q):
        return pltpu.make_async_copy(uf.at[ts, q], uf_out.at[ts, q], fsem.at[ts, q])

    weight = w_ref[...].astype(F32)

    def forward(e_s, stage, etb):
        def etcopy(i):
            cols = pl.ds(pl.multiple_of(vstart + i * EC, LANE), EC)
            return pltpu.make_async_copy(et_ref.at[:, cols], etb.at[:, pl.ds(pl.multiple_of(i * EC, EC), EC)], etsem.at[i])

        start([etcopy(i) for i in range(2 * NP)])
        start([own_ge(half, q) for half in PAIR for q in PAIR])
        ints[0] = jnp.zeros_like(ints[0])
        for half in PAIR:
            for q in PAIR:
                lanes = span(2 * half + q, TB)
                ints[0, half, q, ROW0, :] = tgt_ref[:, lanes] - core * VL
                ints[0, half, q, ROW1, :] = tok_ref[:, lanes] - core * VL
                ints[0, half, q, ROW2, :] = mask_ref[:, lanes]
        hits[...] = jnp.zeros_like(hits)
        for half in PAIR:
            for q in PAIR:
                rows = h_ref[:, pl.ds(half * TS + q * TB, TB)].astype(F32)
                inv = lax.rsqrt(jnp.mean(rows * rows, axis=0, keepdims=True) + RMS_EPS)
                uf[half, q] = rows * inv
        wait([own_ge(half, q) for half in PAIR for q in PAIR])
        for q in PAIR:
            gst[q] = gb[core, q].astype(F32)
        start([keep_ge(q) for q in PAIR])

        def ebody(i, _):
            etcopy(i).wait()
            lanes = pl.ds(pl.multiple_of(i * EC, EC), EC)
            e_s[lanes, :] = etb[:, lanes].T
            return 0

        lax.fori_loop(0, 2 * NP, ebody, 0)
        wait([keep_ge(q) for q in PAIR])
        pl.semaphore_wait(barrier, len(peers))
        start(own[:2])
        start([icopy(d) for d in HOPS])
        start(own[2:])
        iota = lax.broadcasted_iota(I32, (SUB, TB), 0)

        def ocopy(ts, q, slot):
            return pltpu.make_async_copy(stage.at[slot], logit_ref.at[ts, :, pl.ds(pl.multiple_of(q * TB, TB), TB)], osem.at[slot])

        def zt_step(s, _):
            j = four(s)
            r = jnp.where(s < 4, 0, jnp.where(s < 12, 1 + two(j), 3))
            q = jnp.where((s < 8) | (s >= 12), two(j), 1 - two(j))
            half = jnp.where(s < 4, j // 2, jnp.where(j < 2, core, other))
            ts = 2 * r + half

            @pl.when(s == 4)
            def _():
                for i, (r, q) in enumerate(FIRST):
                    own[i].wait_recv()
                    onward[i].start()
                    pcopy(r, q).start()
                arrive([icopy(d) for d in HOPS])
                start(stat_copies(0))
                start(gmine[:2])

            @pl.when(s == 6)
            def _():
                arrive([parrive(r, q) for r, q in FIRST])

            @pl.when(s == 8)
            def _():
                for i, (r, q) in enumerate(LATER):
                    own[2 + i].wait_recv()
                    pcopy(r, q).start()
                count = jnp.sum(ints[:, :, :, 2, :].astype(F32))
                ny[yi] = jnp.full((SUB, LANE), count, F32)
                start(ny_out)

            @pl.when(s == 10)
            def _():
                arrive([parrive(r, q) for r, q in LATER])
                arrive(ny_in)
                nz[zi] = sum4(ny)
                start(nz_out)

            @pl.when(s == 12)
            def _():
                for i in PAIR:
                    onward[i].wait_recv()
                    pcopy(3, i).start()
                start(stat_copies(1) + stat_copies(2))

            @pl.when(s == 14)
            def _():
                arrive([parrive(3, i) for i in PAIR])

            slot = two(s)

            @pl.when(s >= 2)
            def _():
                ocopy(ts, q, slot).wait()

            zt = (uf[ts, q] * weight).astype(BF16)
            zb[ts, q] = zt
            fcopy(ts, q).start()
            tgt = ints[r, half, q, ROW0, :] - vstart
            m8 = jnp.full((SUB, TB), -jnp.inf, F32)
            s8 = jnp.zeros((SUB, TB), F32)
            t8 = jnp.zeros((SUB, TB), F32)
            for vc in range(VB // CH):
                l = jnp.dot(e_s[span(vc, CH), :], zt, preferred_element_type=F32)
                stage[slot, span(vc, CH), :] = l
                mn = m8
                for i in range(CH // SUB):
                    mn = jnp.maximum(mn, l[span(i, SUB)])
                s8 = s8 * jnp.exp(m8 - mn)
                m8 = mn
                for i in range(CH // SUB):
                    li = l[span(i, SUB)]
                    s8 = s8 + jnp.exp(li - mn)
                    t8 = t8 + jnp.where(iota == tgt - (vc * CH + i * SUB), li, 0.0)
            m = jnp.max(m8, axis=0, keepdims=True)
            at_row = 4 * half + 2 * q
            stats[0, r, pl.ds(at_row, 1), :] = m
            stats[0, r, pl.ds(at_row + 1, 1), :] = jnp.sum(s8 * jnp.exp(m8 - m), axis=0, keepdims=True)
            hits[...] += jnp.sum(t8, axis=0, keepdims=True) * ints[r, half, q, ROW2, :].astype(F32)
            ocopy(ts, q, slot).start()
            return 0

        lax.fori_loop(0, NS * 2, zt_step, 0)
        sent(own + onward + [pcopy(r, q) for r in HOPS for q in PAIR])
        wait([fcopy(ts, q) for ts in range(NS) for q in PAIR])
        start(stat_copies(3))
        start(gmine[2:])
        wait([ocopy(0, 0, slot) for slot in PAIR])

    pl.run_scoped(forward, V((VB, D), BF16), V((2, VB, TB), F32), V((D, VB), BF16))

    def backward(dz, de, lbuf, et_s):
        iota = lax.broadcasted_iota(I32, (V2, TS), 0)

        def near_load(vc):
            slot, rows = two(vc), pl.ds(pl.multiple_of(vc * V2, V2), V2)
            cols = pl.ds(pl.multiple_of(vstart + vc * V2, LANE), V2)
            return [
                pltpu.make_async_copy(logit_ref.at[pl.ds(0, NEARS), rows, :], lbuf.at[slot, pl.ds(0, NEARS)], lsem.at[slot, 0]),
                pltpu.make_async_copy(et_ref.at[:, cols], et_s.at[slot, :, pl.ds(0, V2)], esem.at[slot]),
            ]

        def far_load(u, ts=NEARS):
            slot, far = two(u), pl.ds(ts, 2)
            cols = pl.ds(pl.multiple_of(vstart + u * EC, LANE), EC)
            return [
                pltpu.make_async_copy(logit_ref.at[far, pl.ds(pl.multiple_of(u * EC + k * V2, V2), V2), :], lbuf.at[slot, pl.ds(2 * k, 2)], lsem.at[slot, k])
                for k in PAIR
            ] + [pltpu.make_async_copy(et_ref.at[:, cols], et_s.at[slot], esem.at[slot])]

        for slot in PAIR:
            start(far_load(slot))
        dz[...] = jnp.zeros_like(dz)
        arrive(nz_in)
        total = sum4(nz)[ROW0, ROW0]
        for r in QUAD:
            arrive(stat_copies(r))
        loss = -hits[...]
        for r in QUAD:
            for half in PAIR:
                for q in PAIR:
                    lanes = span(q, TB)
                    top, low = (span(4 * half + 2 * q + i, 1) for i in PAIR)
                    ms = [stats[i, r, top, :] for i in range(NS)]
                    m = functools.reduce(jnp.maximum, ms)
                    tot = sum(stats[i, r, low, :] * jnp.exp(ms[i] - m) for i in range(NS))
                    lse = m + jnp.log(tot)
                    mask = ints[r, half, q, ROW2, :].astype(F32)
                    row[2 * r + half, ROW0, lanes] = lse
                    row[2 * r + half, ROW1, lanes] = mask / total
                    ids[2 * r + half, ROW0, lanes] = ints[r, half, q, ROW0, :] - vstart
                    ids[2 * r + half, ROW1, lanes] = ints[r, half, q, ROW1, :] - vstart
                    if r == 0:
                        loss = loss + jnp.where(core == half, mask * lse, 0.0)
        aux[0, ROW1, :] = jnp.broadcast_to(jnp.sum(loss, axis=1, keepdims=True), (1, TB))
        aux[1, ROW1, :] = jnp.broadcast_to(total, (1, TB))

        def piece(p):
            third = p >= 8
            hi = two(p // 2)
            r = jnp.where(third, 3, 1 + hi)
            q = jnp.where(third, hi, jnp.where(p < 4, hi, 1 - hi))
            return 2 * r + two(p), q

        def stage_in(p):
            ts, q = piece(p)
            return pltpu.make_async_copy(gall.at[ts, q], gst.at[two(p)], gsem.at[two(p)])

        def convert(p):
            ts, q = piece(p)
            stage_in(p).wait()
            gb[ts, q] = gst[two(p)].astype(BF16)

        def de_index(u, zblk, qtr):
            return jnp.where(two(u) == 0, zblk * 4 + qtr, qtr * 4 + zblk)

        def dlogits(tile, ts, base):
            p = jnp.exp(tile - row[ts, ROW0, :])
            return (jnp.where(iota == ids[ts, ROW0, :] - base, p - 1.0, p) * row[ts, ROW1, :]).astype(BF16)

        def add_dz(et, ds, ts):
            part = sum(jnp.dot(et[:, span(k, V2)], d, preferred_element_type=F32) for k, d in enumerate(ds))
            for q in PAIR:
                dz[ts % 2, ts // 2, q] += part[:, span(q, TB)]

        def products(et, ds, ts, accs):
            if ts >= 2:
                add_dz(et, ds, ts)
            for q in PAIR:
                for k, d in enumerate(ds):
                    a = lax.dot_general(zb[ts, q], d[:, span(q, TB)], NT, preferred_element_type=F32)
                    accs[k] = a if accs[k] is None else accs[k] + a

        def far_step(u):
            slot, accs = two(u), [None, None]
            wait(far_load(u))
            et = et_s[slot]
            for half in PAIR:
                ts = NEARS + half
                products(et, [dlogits(lbuf[slot, 2 * k + half], ts, u * EC + k * V2) for k in PAIR], ts, accs)
            for zblk in QUAD:
                for qtr in QUAD:
                    de[u, de_index(u, zblk, qtr)] = accs[qtr // 2][span(zblk, ROWS), span(qtr % 2, LANE)]

            @pl.when(u + 2 < 2 * NP)
            def _():
                start(far_load(u + 2))

            @pl.when(u + 2 >= 2 * NP)
            def _():
                start(near_load(u + 2 - 2 * NP))

        def own_step(u):
            slot = two(u)
            wait(far_load(u, 0))
            for half in PAIR:
                add_dz(et_s[slot], [dlogits(lbuf[slot, 2 * k + half], half, u * EC + k * V2) for k in PAIR], half)

            @pl.when(u + 2 < 2 * NP)
            def _():
                start(far_load(u + 2, 0))

        def near_step(vc):
            slot, accs, u = two(vc), [None], vc // 2
            wait(near_load(vc))
            et = et_s[slot, :, span(0, V2)]
            for ts in range(NEARS):
                products(et, [dlogits(lbuf[slot, ts], ts, vc * V2)], ts, accs)
            for zblk in QUAD:
                for ql in PAIR:
                    de[u, de_index(u, zblk, slot * 2 + ql)] += accs[0][span(zblk, ROWS), span(ql, LANE)]

            @pl.when(vc + 2 < N2)
            def _():
                start(near_load(vc + 2))

        def lookup_step(vc):
            base = vc * V2
            acc = None
            for ts in range(NS):
                o = jnp.where(iota == ids[ts, ROW1, :] - base, 1.0, 0.0).astype(BF16)
                for q in PAIR:
                    a = lax.dot_general(gb[ts, q], o[:, span(q, TB)], NT, preferred_element_type=F32)
                    acc = a if acc is None else acc + a
            u = vc // 2
            for zblk in QUAD:
                for ql in PAIR:
                    de[u, de_index(u, zblk, two(vc) * 2 + ql)] += acc[span(zblk, ROWS), span(ql, LANE)]

        def lookups(first):
            def one(i, _):
                lookup_step(first + i)
                return 0

            lax.fori_loop(0, 4, one, 0)

        def unit(p, c):
            return 2 * p + c

        def a1(p, c):
            a, _ = AXES[c]
            k, op = two(p), at(a, 2) * 4
            return [remote(de.at[unit(p, c), pl.ds(op + 2 * i, 2)], ra1.at[c, k, i], a1s.at[c, k, i], a1r.at[c, k, i], hop(a, i)) for i in PAIR]

        def a2(p, c):
            a, _ = AXES[c]
            k = two(p)
            return [remote(de.at[unit(p, c), pl.ds(at(a, side(i)) * 4, 4)], ra2.at[c, k, i], a2s.at[c, k, i], a2r.at[c, k, i], hop(a, i)) for i in PAIR]

        def b1(p, c):
            a, b = AXES[c]
            k, i2 = two(p), me[a] * 4 + at(b, 2)
            return [remote(de.at[unit(p, c), i2, pl.ds(HROWS * i, HROWS)], rb1.at[c, k, i], b1s.at[c, k, i], b1r.at[c, k, i], hop(b, i)) for i in PAIR]

        def b2(p, c):
            a, b = AXES[c]
            k = two(p)
            return [remote(de.at[unit(p, c), me[a] * 4 + at(b, side(i))], rb2.at[c, k, i], b2s.at[c, k, i], b2r.at[c, k, i], hop(b, i)) for i in PAIR]

        def do_a1(p):
            for c in PAIR:
                start(a1(p, c))

        def do_a2(p):
            k = two(p)
            for c in PAIR:
                a, _ = AXES[c]
                wait(a1(p, c))
                for i in PAIR:
                    for j in PAIR:
                        de[unit(p, c), at(a, side(i)) * 4 + 2 * i + j] += ra1[c, k, i, j]
                start(a2(p, c))

        def do_b1(p):
            k = two(p)
            for c in PAIR:
                a, _ = AXES[c]
                wait(a2(p, c))
                for j in QUAD:
                    de[unit(p, c), me[a] * 4 + j] += ra2[c, k, 0, j] + ra2[c, k, 1, j]
                start(b1(p, c))

        def do_b2(p):
            k = two(p)
            for c in PAIR:
                a, b = AXES[c]
                wait(b1(p, c))
                for i in PAIR:
                    de[unit(p, c), me[a] * 4 + at(b, side(i)), span(i, HROWS)] += rb1[c, k, i]
                start(b2(p, c))

        def do_f(p):
            k = two(p)
            for c in PAIR:
                a, b = AXES[c]
                wait(b2(p, c))
                de[unit(p, c), me[a] * 4 + me[b]] += rb2[c, k, 0] + rb2[c, k, 1]

        def col(b, dy, dx):
            dst = at("y", dy) * 4 + at("x", dx)
            return remote(sb.at[b, dst], rv.at[b, yi * 4 + xi], ass.at[b, dy * 4 + dx], asr.at[b, dy * 4 + dx], {"y": at("y", dy), "x": at("x", dx)})

        def col_arrive(b, dy, dx):
            src = at("y", -dy % 4) * 4 + at("x", -dx % 4)
            return remote(sb.at[b, src], rv.at[b, src], ass.at[b, dy * 4 + dx], asr.at[b, dy * 4 + dx], {"y": at("y", dy), "x": at("x", dx)})

        def out_de(b, x):
            lanes = pl.ds(x * VB + b * 4 * EC, 4 * EC)
            return pltpu.make_async_copy(de_s.at[:, lanes], de_out.at[:, lanes], desem.at[b, x])

        def do_cols(b):
            for k in QUAD:
                first, second = AXES[k % 2]
                mine = me[first] * 4 + me[second]
                for s in range(16):
                    sb[b, s, span(k, OWN), :] = de[4 * b + k, mine, span(s, OWN), :]
            start([col(b, dy, dx) for dy, dx in FAR])
            rv[b, yi * 4 + xi] = sb[b, yi * 4 + xi]

        def do_assemble(b):
            arrive([col_arrive(b, dy, dx) for dy, dx in FAR])
            for s in range(16):
                for k in QUAD:
                    lane = (s % 4) * VB + (4 * b + k) * EC + (s // 4) * LANE
                    de_s[:, pl.ds(lane, LANE)] = rv[b, s, span(k, OWN), :]
            start([out_de(b, x) for x in QUAD])

        def dcopy(r):
            return remote(dz.at[other, r], uf.at[r], dps.at[r], dpr.at[r], {"tp": other})

        def unit_in(r, q):
            return pltpu.make_async_copy(uf_out.at[2 * r + core, q], gst.at[q], gsem.at[q])

        def fetch(r):
            start([unit_in(r, q) for q in PAIR])

        def core_sum(r):
            dcopy(r).wait_recv()
            for q in PAIR:
                dz[core, r, q] += uf[r, q]

        def gain_sum(r):
            wait([unit_in(r, q) for q in PAIR])
            dg = gain[...]
            for q in PAIR:
                for j in PAIR:
                    dg = dg + dz[core, r, q, :, span(j, LANE)] * gst[q, :, span(j, LANE)]
            gain[...] = dg

        def c1(i, q):
            return remote(dz.at[core, 3, q, pl.ds(HD * i, HD)], uf.at[6, i, pl.ds(HD * q, HD)], c1s.at[i, q], c1r.at[i, q], hop("x", i))

        def c2(i):
            return remote(dz.at[core, 2 - i], uf.at[4 + i], c2s.at[i], c2r.at[i], hop("x", i))

        def far_unit(u, _):
            @pl.when(u == 2)
            def _():
                for i, (r, q) in enumerate(FIRST):
                    gmine[i].wait_recv()
                    gonward[i].start()
                    gpcopy(r, q).start()

            @pl.when(u == 4)
            def _():
                arrive([gparrive(r, q) for r, q in FIRST])
                start([stage_in(p) for p in PAIR])

            @pl.when(u == 8)
            def _():
                for i, (r, q) in enumerate(LATER):
                    gmine[2 + i].wait_recv()
                    gpcopy(r, q).start()

            @pl.when(u == 10)
            def _():
                arrive([gparrive(r, q) for r, q in LATER])
                start([stage_in(4 + p) for p in PAIR])

            @pl.when((u >= 5) & (u < 9))
            def _():
                convert(u - 5)

            @pl.when((u >= 5) & (u < 7))
            def _():
                stage_in(u - 3).start()

            @pl.when(u == 11)
            def _():
                convert(4)
                stage_in(6).start()

            far_step(u)
            return 0

        lax.fori_loop(0, 2 * NP, far_unit, 0)
        dcopy(3).start()

        def near_chunk(vc, _):
            @pl.when(vc == 0)
            def _():
                convert(5)
                stage_in(7).start()

            @pl.when((vc >= 1) & (vc < 3))
            def _():
                convert(vc + 5)

            @pl.when(vc == 2)
            def _():
                core_sum(3)
                start([c1(i, q) for i in PAIR for q in PAIR])

            @pl.when(vc == 3)
            def _():
                for i in PAIR:
                    gonward[i].wait_recv()
                    gpcopy(3, i).start()

            near_step(vc)
            return 0

        lax.fori_loop(0, NA, near_chunk, 0)
        arrive([gparrive(3, i) for i in PAIR])
        start([stage_in(8 + p) for p in PAIR])
        for p in range(8, 12):
            convert(p)
            if p < 10:
                stage_in(p + 2).start()

        def phase_c(p, _):
            @pl.when(p >= 1)
            def _():
                do_a2(p - 1)

            lookups(4 * p)

            @pl.when(p >= 2)
            def _():
                do_b2(p - 2)

            do_a1(p)

            @pl.when(p == 4)
            def _():
                do_cols(0)

            def more(i, _):
                near_step(NA + 4 * p + i)
                return 0

            lax.fori_loop(0, 4, more, 0)

            @pl.when(p >= 2)
            def _():
                do_f(p - 2)

            @pl.when(p >= 1)
            def _():
                do_b1(p - 1)

            return 0

        lax.fori_loop(0, NP - 1, phase_c, 0)

        start([dcopy(r) for r in (1, 2)])
        fetch(1)
        for slot in PAIR:
            start(far_load(slot, 0))
        do_a2(4)
        gain[...] = jnp.zeros_like(gain)

        def to_neighbour(i):
            core_sum(2 - i)
            for q in PAIR:
                c1(i, q).wait()
                dz[core, 2 - i, q, span(i, HD)] += uf[6, i, span(q, HD)]
            c2(i).start()

        def last_lookups(i, _):
            lookup_step(20 + i)

            @pl.when(i == 0)
            def _():
                to_neighbour(1)

            @pl.when(i == 1)
            def _():
                to_neighbour(0)

            @pl.when(i == 2)
            def _():
                gain_sum(1)
                fetch(2)

            return 0

        lax.fori_loop(0, 4, last_lookups, 0)
        do_b2(3)
        do_a1(5)

        def own_unit(u, _):
            @pl.when(u == 1)
            def _():
                do_b1(4)

            @pl.when(u == 2)
            def _():
                gain_sum(2)
                fetch(0)

            @pl.when(u == 5)
            def _():
                do_b2(4)
                do_a2(5)

            @pl.when(u == 8)
            def _():
                do_f(3)
                do_cols(1)

            own_step(u)
            return 0

        lax.fori_loop(0, 2 * NP, own_unit, 0)
        dcopy(0).start()
        do_f(4)
        core_sum(0)
        gain_sum(0)
        st[core] = jnp.zeros(SUMS, F32)
        st[core, ROW0, span(0, D)] = jnp.sum(gain[...].T, axis=0, keepdims=True)
        st[core, ROW1, span(0, TB)] = aux[0, ROW1, :]
        pair_copy = remote(st.at[core], st.at[core], sts, str_, {"tp": other})
        pair_arrive = remote(st.at[core], st.at[other], sts, str_, {"tp": other})
        pair_copy.start()
        sums = [gather_axis(buf, axis, sas.at[k], sar.at[k]) for k, (buf, axis) in enumerate(((sz, "z"), (sy, "y"), (sx, "x")))]
        do_b1(5)
        pair_arrive.wait()
        sz[zi] = st[0] + st[1]
        start(sums[0][0])
        do_assemble(0)
        do_b2(5)
        wait(sums[0][1])
        sy[yi] = sum4(sz)
        start(sums[1][0])
        do_f(5)
        do_cols(2)
        wait(sums[1][1])
        sx[xi] = sum4(sy)
        start(sums[2][0])
        do_assemble(1)

        for q in PAIR:
            rows = h_ref[:, pl.ds(pl.multiple_of(core * TS + q * TB, TB), TB)].astype(F32)
            inv = lax.rsqrt(jnp.mean(rows * rows, axis=0, keepdims=True) + RMS_EPS)
            gst[q] = rows * inv
            aux[q, ROW0, :] = inv
        wait([c2(i) for i in PAIR])
        for q in PAIR:
            unit, inv = gst[q], aux[q, ROW0, :]
            gu = (dz[core, 0, q] + uf[4, q] + uf[5, q]) * weight
            dz[core, 3, q] = inv * (gu - unit * jnp.mean(gu * unit, axis=0, keepdims=True))
        half_copy = remote(dz.at[core, 3], uf.at[7], hs, hr, {"tp": other})
        half_copy.start()
        wait(sums[2][1])
        sum_out[...] = sum4(sx)
        sum_out[ROW1, span(0, TB)] = sum_out[ROW1, span(0, TB)] / aux[1, ROW1, :]
        half_copy.wait()
        for half in PAIR:
            for q in PAIR:
                gb[half, q] = jnp.where(core == half, dz[core, 3, q], uf[7, q]).astype(BF16)
                out_dh(half, q).start()
        do_assemble(2)
        wait([out_dh(half, q) for half in PAIR for q in PAIR])
        wait([out_de(b, x) for b in BATCHES for x in QUAD])

        sent(gmine + gonward + [gpcopy(r, q) for r in HOPS for q in PAIR] + [dcopy(r) for r in QUAD])
        sent([col(b, dy, dx) for b in BATCHES for dy, dx in FAR])
    pl.run_scoped(
        backward, V((2, GX, 2, D, TB), F32), V((2 * NP, 16, ROWS, LANE), F32), V((2, NS, V2, TS), F32), V((2, D, EC), BF16)
    )
    sent([icopy(d) for d in HOPS] + ny_out + nz_out)
    for r in QUAD:
        sent(stat_copies(r))


def call(*args):
    links = [DMA((2, 2, 2))] * 8
    return pl.pallas_call(
        kernel,
        out_shape=(
            SDS((OWN, VL), F32), SDS((D, TOK), BF16), SDS(SUMS, F32),
            SDS((NS, VB, TS), F32), SDS(TOKENS, F32), SDS(TOKENS, F32),
        ),
        in_specs=[VMEM, ANY] + [VMEM] * 4 + [ANY],
        out_specs=(ANY, ANY, VMEM) + (ANY,) * 3,
        scratch_shapes=[
            V(TOKENS, F32),
            *[V(TOKENS, BF16)] * 2,
            V((2, D, TB), F32),
            V((GX, 2, 2, SUB, TB), I32),
            V((NS, GX, SUB, TB), F32), V((1, TB), F32),
            *[V((GX, SUB, LANE), F32)] * 2,
            V((NS, 2, TS), F32), V((NS, 2, TS), I32), V((2, SUB, TB), F32),
            V((D, LANE), F32),
            V((OWN, VL), F32),
            V((2, 2, 2, 2, ROWS, LANE), F32),
            V((2, 2, 2, GX, ROWS, LANE), F32),
            V((2, 2, 2, HROWS, LANE), F32),
            V((2, 2, 2, ROWS, LANE), F32),
            *[V((3, 16, 40, LANE), F32)] * 2,
            V((2, *SUMS), F32), *[V((GX, *SUMS), F32)] * 3,
            DMA((3, GX)), DMA((2 * NP,)), DMA((2,)), DMA((2, 2)), *[DMA((2,))] * 2, DMA((2, 2)), *[DMA((NS, 2))] * 2,
            DMA((NS,)), *[DMA((GX, 2))] * 3, *[DMA((GX,))] * 2, *[DMA((NS, GX))] * 2, *[DMA((2, GX))] * 2,
            DMA((NS,)), *[DMA((GX, 2))] * 3, *links,
            *[DMA((3, 16))] * 2, *[DMA((GX,))] * 2, *[DMA((2, 2))] * 2, *[DMA((2,))] * 2, *[DMA(())] * 4, *[DMA((3, GX))] * 2,
        ],
        compiler_params=pltpu.CompilerParams(vmem_limit_bytes=67043328, collective_id=0, has_side_effects=True),
    )(*args)


def solution(mesh):
    mesh4 = Mesh(mesh.devices.reshape(2, GX, GX, GX), ("tp", "z", "y", "x"))

    def local_step(hidden, norm_w, embed, targets, loss_mask, token_ids, grad_embed):
        h_t = hidden.reshape(TOK, D).T
        ge_t = grad_embed.reshape(TOK, D).T
        de, dh, sums, *_ = call(h_t, ge_t, norm_w.reshape(D, 1), targets, loss_mask, token_ids, embed.T)
        return sums[1, 0], dh.T.reshape(hidden.shape), sums[0, :D], de.T

    dp = ("z", "y", "x")
    return jax.shard_map(
        local_step,
        mesh=mesh4,
        in_specs=(P(dp), P(), P("tp"), P(dp), P(dp), P(dp), P(dp)),
        out_specs=(P(), P(dp), P(), P("tp", dp)),
        check_vma=False,
    )
```

```python
import functools

import jax
import jax.numpy as jnp
from jax import lax
from jax.experimental import pallas as pl
from jax.experimental.pallas import tpu as pltpu
from jax.sharding import Mesh, PartitionSpec as P

RMS_EPS = 1e-6
F32, BF16, I32 = jnp.float32, jnp.bfloat16, jnp.int32
MESH = pl.DeviceIdType.MESH
D = 576
TOK = 1024
GX = 4
VL = 24576
VB = VL // GX
TS = 512
TB = 256
NS = GX * 2
V2 = 256
N2 = VB // V2
CH = 256
ROWS, LANE, OWN = 144, 128, 9
HROWS, HD, EC = ROWS // 2, D // 2, 512
VMEM = pl.BlockSpec(memory_space=pltpu.VMEM)
ANY = pl.BlockSpec(memory_space=pl.ANY)
V, DMA, SDS = pltpu.VMEM, pltpu.SemaphoreType.DMA, jax.ShapeDtypeStruct
SUB = 8
TOKENS = (NS, 2, D, TB)
SUMS = (2, 640)
GRID = [(dy, dx) for dy in range(4) for dx in range(4)]
FAR = GRID[1:]
GROUP = [(d, cross) for d in range(4) for cross in range(2) if d or cross]
PAIR, QUAD = range(2), range(4)
HOPS = QUAD[1:]
ROW0, ROW1, ROW2 = (slice(i, i + 1) for i in range(3))
NT = (((1,), (1,)), ((), ()))
FIRST, LATER = ((1, 0), (2, 1)), ((1, 1), (2, 0))
DELTA = (0, 3, 1, 2)
SLOT = [DELTA.index(d) for d in QUAD]


def span(i, n):
    return slice(i * n, i * n + n)


def sum4(buf):
    return (buf[0] + buf[1]) + (buf[2] + buf[3])


def two(n):
    return lax.rem(n, 2)


def four(n):
    return lax.rem(n, 4)


def side(i):
    return 1 + 2 * i


def remote(src, dst, send, recv, where):
    return pltpu.make_async_remote_copy(src_ref=src, dst_ref=dst, send_sem=send, recv_sem=recv, device_id=where, device_id_type=MESH)


NEARS, BATCHES = NS - 2, range(3)
NP = 6
NA = 4
AXES = ("zy", "yz")


def kernel(
    h_ref, ge_ref, w_ref, tgt_ref, mask_ref, tok_ref, et_ref,
    de_out, dh_out, sum_out, logit_ref, uf_out, gall,
    uf, zb, gb, gst, ints, stats, hits, ny, nz, row, ids, aux,
    gain, de_s, ra1, ra2, rb1, rb2, sb, rv, st, sx, sy, sz,
    desem, etsem, osem, lsem, esem, gsem, gown, zsem, fsem,
    usend, urecv, psend, precv, isend, irecv, ssend, srecv, nsend, nrecv,
    gsend, grecv, gpsend, gprecv, a1s, a1r, a2s, a2r, b1s, b1r, b2s, b2r,
    ass, asr, dps, dpr, c1s, c1r, c2s, c2r, hs, hr, sts, str_, sas, sar,
):
    core = lax.axis_index("tp")
    me = {axis: lax.axis_index(axis) for axis in "xyz"}
    xi, yi, zi = (me[axis] for axis in "xyz")
    other = 1 - core
    vstart = xi * VB

    def at(axis, d):
        return four(me[axis] + d)

    def hop(axis, i):
        return {axis: at(axis, side(i))}

    barrier = pltpu.get_barrier_semaphore()
    peers = [{"y": at("y", dy), "x": at("x", dx)} for dy, dx in FAR]
    peers += [{"z": at("z", d)} for d in HOPS] + [{"x": at("x", d), "tp": other} for d in QUAD]
    for peer in peers:
        pl.semaphore_signal(barrier, inc=1, device_id=peer, device_id_type=MESH)

    def start(copies):
        for copy in copies:
            copy.start()

    def wait(copies):
        for copy in copies:
            copy.wait()

    def arrive(copies):
        for copy in copies:
            copy.wait_recv()

    def sent(copies):
        for copy in copies:
            copy.wait_send()

    right, left = at("x", 1), at("x", 3)
    ways = (left, right)

    def ucopy(src, q, dst, way, index):
        return remote(uf.at[2 * src + core, q], uf.at[2 * dst + core, q], usend.at[index], urecv.at[dst, q], {"x": way})

    def pcopy(r, q):
        return remote(uf.at[2 * r + core, q], uf.at[2 * r + core, q], psend.at[r, q], precv.at[r, q], {"tp": other})

    def parrive(r, q):
        return remote(uf.at[2 * r + core, q], uf.at[2 * r + other, q], psend.at[r, q], precv.at[r, q], {"tp": other})

    own = [ucopy(0, q, r, ways[r % 2], i) for i, (r, q) in enumerate(FIRST + LATER)]
    onward = [ucopy(r, q, 3, ways[r % 2], 4 + q) for r, q in FIRST]

    def gcopy(src, q, dst, way, index):
        return remote(gall.at[2 * src + core, q], gall.at[2 * dst + core, q], gsend.at[index], grecv.at[dst, q], {"x": way})

    def gpcopy(r, q):
        return remote(gall.at[2 * r + core, q], gall.at[2 * r + core, q], gpsend.at[r, q], gprecv.at[r, q], {"tp": other})

    def gparrive(r, q):
        return remote(gall.at[2 * r + core, q], gall.at[2 * r + other, q], gpsend.at[r, q], gprecv.at[r, q], {"tp": other})

    gmine = [gcopy(0, q, r, ways[r % 2], i) for i, (r, q) in enumerate(FIRST + LATER)]
    gonward = [gcopy(r, q, 3, ways[r % 2], 4 + q) for r, q in FIRST]

    def own_ge(half, q):
        return pltpu.make_async_copy(ge_ref.at[:, pl.ds(half * TS + q * TB, TB)], gb.at[half, q], gown.at[half, q])

    def out_dh(half, q):
        return pltpu.make_async_copy(gb.at[half, q], dh_out.at[:, pl.ds(half * TS + q * TB, TB)], gown.at[half, q])

    def keep_ge(q):
        return pltpu.make_async_copy(gst.at[q], gall.at[core, q], gsem.at[q])

    def icopy(d):
        return remote(ints.at[0], ints.at[SLOT[-d % 4]], isend.at[d], irecv.at[SLOT[-d % 4]], {"x": at("x", d)})

    def scopy(r, d, cross):
        index = 2 * d + cross
        where = {"x": at("x", d), "tp": other} if cross else {"x": at("x", d)}
        dst = SLOT[(DELTA[r] - d) % 4]
        return remote(stats.at[0, r], stats.at[index, dst], ssend.at[index, r], srecv.at[index, dst], where)

    def stat_copies(r):
        return [scopy(r, d, cross) for d, cross in GROUP]

    def gather_axis(buf, axis, sends, recvs):
        mine = me[axis]
        out = [remote(buf.at[mine], buf.at[mine], sends.at[d], recvs.at[d], {axis: at(axis, d)}) for d in HOPS]
        back = [remote(buf.at[mine], buf.at[at(axis, -d % 4)], sends.at[d], recvs.at[d], {axis: at(axis, d)}) for d in HOPS]
        return out, back

    ny_out, ny_in = gather_axis(ny, "y", nsend.at[0], nrecv.at[0])
    nz_out, nz_in = gather_axis(nz, "z", nsend.at[1], nrecv.at[1])

    def fcopy(ts, q):
        return pltpu.make_async_copy(uf.at[ts, q], uf_out.at[ts, q], fsem.at[ts, q])

    weight = w_ref[...].astype(F32)

    def forward(e_s, stage, etb):
        def etcopy(i):
            cols = pl.ds(pl.multiple_of(vstart + i * EC, LANE), EC)
            return pltpu.make_async_copy(et_ref.at[:, cols], etb.at[:, pl.ds(pl.multiple_of(i * EC, EC), EC)], etsem.at[i])

        start([etcopy(i) for i in range(2 * NP)])
        start([own_ge(half, q) for half in PAIR for q in PAIR])
        ints[0] = jnp.zeros_like(ints[0])
        for half in PAIR:
            for q in PAIR:
                lanes = span(2 * half + q, TB)
                ints[0, half, q, ROW0, :] = tgt_ref[:, lanes] - core * VL
                ints[0, half, q, ROW1, :] = tok_ref[:, lanes] - core * VL
                ints[0, half, q, ROW2, :] = mask_ref[:, lanes]
        hits[...] = jnp.zeros_like(hits)
        for half in PAIR:
            for q in PAIR:
                rows = h_ref[:, pl.ds(half * TS + q * TB, TB)].astype(F32)
                inv = lax.rsqrt(jnp.mean(rows * rows, axis=0, keepdims=True) + RMS_EPS)
                uf[half, q] = rows * inv

        def ebody(i, _):
            etcopy(i).wait()
            lanes = pl.ds(pl.multiple_of(i * EC, EC), EC)
            e_s[lanes, :] = etb[:, lanes].T
            return 0

        lax.fori_loop(0, 2 * NP, ebody, 0)
        pl.semaphore_wait(barrier, len(peers))
        start(own[:2])
        start([icopy(d) for d in HOPS])
        start(own[2:])
        wait([own_ge(half, q) for half in PAIR for q in PAIR])
        for q in PAIR:
            gst[q] = gb[core, q].astype(F32)
        start([keep_ge(q) for q in PAIR])
        iota = lax.broadcasted_iota(I32, (SUB, TB), 0)

        def ocopy(ts, q, slot):
            return pltpu.make_async_copy(stage.at[slot], logit_ref.at[ts, :, pl.ds(pl.multiple_of(q * TB, TB), TB)], osem.at[slot])

        def zt_step(s, _):
            j = four(s)
            r = jnp.where(s < 4, 0, jnp.where(s < 12, 1 + two(j), 3))
            q = jnp.where((s < 8) | (s >= 12), two(j), 1 - two(j))
            half = jnp.where(s < 4, j // 2, jnp.where(j < 2, core, other))
            ts = 2 * r + half

            @pl.when(s == 4)
            def _():
                for i, (r, q) in enumerate(FIRST):
                    own[i].wait_recv()
                    onward[i].start()
                    pcopy(r, q).start()
                arrive([icopy(d) for d in HOPS])
                start(stat_copies(0))
                wait([keep_ge(q) for q in PAIR])
                start(gmine[:2])

            @pl.when(s == 6)
            def _():
                arrive([parrive(r, q) for r, q in FIRST])

            @pl.when(s == 8)
            def _():
                for i, (r, q) in enumerate(LATER):
                    own[2 + i].wait_recv()
                    pcopy(r, q).start()
                count = jnp.sum(ints[:, :, :, 2, :].astype(F32))
                ny[yi] = jnp.full((SUB, LANE), count, F32)
                start(ny_out)

            @pl.when(s == 10)
            def _():
                arrive([parrive(r, q) for r, q in LATER])
                arrive(ny_in)
                nz[zi] = sum4(ny)
                start(nz_out)

            @pl.when(s == 12)
            def _():
                for i in PAIR:
                    onward[i].wait_recv()
                    pcopy(3, i).start()
                start(stat_copies(1) + stat_copies(2))

            @pl.when(s == 14)
            def _():
                arrive([parrive(3, i) for i in PAIR])

            slot = two(s)

            @pl.when(s >= 2)
            def _():
                ocopy(ts, q, slot).wait()

            zt = (uf[ts, q] * weight).astype(BF16)
            zb[ts, q] = zt
            fcopy(ts, q).start()
            tgt = ints[r, half, q, ROW0, :] - vstart
            m8 = jnp.full((SUB, TB), -jnp.inf, F32)
            s8 = jnp.zeros((SUB, TB), F32)
            t8 = jnp.zeros((SUB, TB), F32)
            for vc in range(VB // CH):
                l = jnp.dot(e_s[span(vc, CH), :], zt, preferred_element_type=F32)
                stage[slot, span(vc, CH), :] = l
                mn = m8
                for i in range(CH // SUB):
                    mn = jnp.maximum(mn, l[span(i, SUB)])
                s8 = s8 * jnp.exp(m8 - mn)
                m8 = mn
                for i in range(CH // SUB):
                    li = l[span(i, SUB)]
                    s8 = s8 + jnp.exp(li - mn)
                    t8 = t8 + jnp.where(iota == tgt - (vc * CH + i * SUB), li, 0.0)
            m = jnp.max(m8, axis=0, keepdims=True)
            at_row = 4 * half + 2 * q
            stats[0, r, pl.ds(at_row, 1), :] = m
            stats[0, r, pl.ds(at_row + 1, 1), :] = jnp.sum(s8 * jnp.exp(m8 - m), axis=0, keepdims=True)
            hits[...] += jnp.sum(t8, axis=0, keepdims=True) * ints[r, half, q, ROW2, :].astype(F32)
            ocopy(ts, q, slot).start()
            return 0

        lax.fori_loop(0, NS * 2, zt_step, 0)
        sent(own + onward + [pcopy(r, q) for r in HOPS for q in PAIR])
        wait([fcopy(ts, q) for ts in range(NS) for q in PAIR])
        start(stat_copies(3))
        start(gmine[2:])
        wait([ocopy(0, 0, slot) for slot in PAIR])

    pl.run_scoped(forward, V((VB, D), BF16), V((2, VB, TB), F32), V((D, VB), BF16))

    def backward(dz, de, lbuf, et_s):
        iota = lax.broadcasted_iota(I32, (V2, TS), 0)

        def near_load(vc):
            slot, rows = two(vc), pl.ds(pl.multiple_of(vc * V2, V2), V2)
            cols = pl.ds(pl.multiple_of(vstart + vc * V2, LANE), V2)
            return [
                pltpu.make_async_copy(logit_ref.at[pl.ds(0, NEARS), rows, :], lbuf.at[slot, pl.ds(0, NEARS)], lsem.at[slot, 0]),
                pltpu.make_async_copy(et_ref.at[:, cols], et_s.at[slot, :, pl.ds(0, V2)], esem.at[slot]),
            ]

        def far_load(u, ts=NEARS):
            slot, far = two(u), pl.ds(ts, 2)
            cols = pl.ds(pl.multiple_of(vstart + u * EC, LANE), EC)
            return [
                pltpu.make_async_copy(logit_ref.at[far, pl.ds(pl.multiple_of(u * EC + k * V2, V2), V2), :], lbuf.at[slot, pl.ds(2 * k, 2)], lsem.at[slot, k])
                for k in PAIR
            ] + [pltpu.make_async_copy(et_ref.at[:, cols], et_s.at[slot], esem.at[slot])]

        for slot in PAIR:
            start(far_load(slot))
        dz[...] = jnp.zeros_like(dz)
        arrive(nz_in)
        total = sum4(nz)[ROW0, ROW0]
        for r in QUAD:
            arrive(stat_copies(r))
        loss = -hits[...]
        for r in QUAD:
            for half in PAIR:
                for q in PAIR:
                    lanes = span(q, TB)
                    top, low = (span(4 * half + 2 * q + i, 1) for i in PAIR)
                    ms = [stats[i, r, top, :] for i in range(NS)]
                    m = functools.reduce(jnp.maximum, ms)
                    tot = sum(stats[i, r, low, :] * jnp.exp(ms[i] - m) for i in range(NS))
                    lse = m + jnp.log(tot)
                    mask = ints[r, half, q, ROW2, :].astype(F32)
                    row[2 * r + half, ROW0, lanes] = lse
                    row[2 * r + half, ROW1, lanes] = mask / total
                    ids[2 * r + half, ROW0, lanes] = ints[r, half, q, ROW0, :] - vstart
                    ids[2 * r + half, ROW1, lanes] = ints[r, half, q, ROW1, :] - vstart
                    if r == 0:
                        loss = loss + jnp.where(core == half, mask * lse, 0.0)
        aux[0, ROW1, :] = jnp.broadcast_to(jnp.sum(loss, axis=1, keepdims=True), (1, TB))
        aux[1, ROW1, :] = jnp.broadcast_to(total, (1, TB))

        def piece(p):
            third = p >= 8
            hi = two(p // 2)
            r = jnp.where(third, 3, 1 + hi)
            q = jnp.where(third, hi, jnp.where(p < 4, hi, 1 - hi))
            return 2 * r + two(p), q

        def stage_in(p):
            ts, q = piece(p)
            return pltpu.make_async_copy(gall.at[ts, q], gst.at[two(p)], gsem.at[two(p)])

        def convert(p):
            ts, q = piece(p)
            stage_in(p).wait()
            gb[ts, q] = gst[two(p)].astype(BF16)

        def de_index(u, zblk, qtr):
            return jnp.where(two(u) == 0, zblk * 4 + qtr, qtr * 4 + zblk)

        def dlogits(tile, ts, base):
            p = jnp.exp(tile - row[ts, ROW0, :])
            return (jnp.where(iota == ids[ts, ROW0, :] - base, p - 1.0, p) * row[ts, ROW1, :]).astype(BF16)

        def add_dz(et, ds, ts):
            part = sum(jnp.dot(et[:, span(k, V2)], d, preferred_element_type=F32) for k, d in enumerate(ds))
            for q in PAIR:
                dz[ts % 2, ts // 2, q] += part[:, span(q, TB)]

        def products(et, ds, ts, accs):
            if ts >= 2:
                add_dz(et, ds, ts)
            for q in PAIR:
                for k, d in enumerate(ds):
                    a = lax.dot_general(zb[ts, q], d[:, span(q, TB)], NT, preferred_element_type=F32)
                    accs[k] = a if accs[k] is None else accs[k] + a

        def far_step(u):
            slot, accs = two(u), [None, None]
            wait(far_load(u))
            et = et_s[slot]
            for half in PAIR:
                ts = NEARS + half
                products(et, [dlogits(lbuf[slot, 2 * k + half], ts, u * EC + k * V2) for k in PAIR], ts, accs)
            for zblk in QUAD:
                for qtr in QUAD:
                    de[u, de_index(u, zblk, qtr)] = accs[qtr // 2][span(zblk, ROWS), span(qtr % 2, LANE)]

            @pl.when(u + 2 < 2 * NP)
            def _():
                start(far_load(u + 2))

            @pl.when(u + 2 >= 2 * NP)
            def _():
                start(near_load(u + 2 - 2 * NP))

        def own_step(u):
            slot = two(u)
            wait(far_load(u, 0))
            for half in PAIR:
                add_dz(et_s[slot], [dlogits(lbuf[slot, 2 * k + half], half, u * EC + k * V2) for k in PAIR], half)

            @pl.when(u + 2 < 2 * NP)
            def _():
                start(far_load(u + 2, 0))

        def near_step(vc):
            slot, accs, u = two(vc), [None], vc // 2
            wait(near_load(vc))
            et = et_s[slot, :, span(0, V2)]
            for ts in range(NEARS):
                products(et, [dlogits(lbuf[slot, ts], ts, vc * V2)], ts, accs)
            for zblk in QUAD:
                for ql in PAIR:
                    de[u, de_index(u, zblk, slot * 2 + ql)] += accs[0][span(zblk, ROWS), span(ql, LANE)]

            @pl.when(vc + 2 < N2)
            def _():
                start(near_load(vc + 2))

        def lookup_step(vc):
            base = vc * V2
            acc = None
            for ts in range(NS):
                o = jnp.where(iota == ids[ts, ROW1, :] - base, 1.0, 0.0).astype(BF16)
                for q in PAIR:
                    a = lax.dot_general(gb[ts, q], o[:, span(q, TB)], NT, preferred_element_type=F32)
                    acc = a if acc is None else acc + a
            u = vc // 2
            for zblk in QUAD:
                for ql in PAIR:
                    de[u, de_index(u, zblk, two(vc) * 2 + ql)] += acc[span(zblk, ROWS), span(ql, LANE)]

        def lookups(first):
            def one(i, _):
                lookup_step(first + i)
                return 0

            lax.fori_loop(0, 4, one, 0)

        def unit(p, c):
            return 2 * p + c

        def a1(p, c):
            a, _ = AXES[c]
            k, op = two(p), at(a, 2) * 4
            return [remote(de.at[unit(p, c), pl.ds(op + 2 * i, 2)], ra1.at[c, k, i], a1s.at[c, k, i], a1r.at[c, k, i], hop(a, i)) for i in PAIR]

        def a2(p, c):
            a, _ = AXES[c]
            k = two(p)
            return [remote(de.at[unit(p, c), pl.ds(at(a, side(i)) * 4, 4)], ra2.at[c, k, i], a2s.at[c, k, i], a2r.at[c, k, i], hop(a, i)) for i in PAIR]

        def b1(p, c):
            a, b = AXES[c]
            k, i2 = two(p), me[a] * 4 + at(b, 2)
            return [remote(de.at[unit(p, c), i2, pl.ds(HROWS * i, HROWS)], rb1.at[c, k, i], b1s.at[c, k, i], b1r.at[c, k, i], hop(b, i)) for i in PAIR]

        def b2(p, c):
            a, b = AXES[c]
            k = two(p)
            return [remote(de.at[unit(p, c), me[a] * 4 + at(b, side(i))], rb2.at[c, k, i], b2s.at[c, k, i], b2r.at[c, k, i], hop(b, i)) for i in PAIR]

        def do_a1(p):
            for c in PAIR:
                start(a1(p, c))

        def do_a2(p):
            k = two(p)
            for c in PAIR:
                a, _ = AXES[c]
                wait(a1(p, c))
                for i in PAIR:
                    for j in PAIR:
                        de[unit(p, c), at(a, side(i)) * 4 + 2 * i + j] += ra1[c, k, i, j]
                start(a2(p, c))

        def do_b1(p):
            k = two(p)
            for c in PAIR:
                a, _ = AXES[c]
                wait(a2(p, c))
                for j in QUAD:
                    de[unit(p, c), me[a] * 4 + j] += ra2[c, k, 0, j] + ra2[c, k, 1, j]
                start(b1(p, c))

        def do_b2(p):
            k = two(p)
            for c in PAIR:
                a, b = AXES[c]
                wait(b1(p, c))
                for i in PAIR:
                    de[unit(p, c), me[a] * 4 + at(b, side(i)), span(i, HROWS)] += rb1[c, k, i]
                start(b2(p, c))

        def do_f(p):
            k = two(p)
            for c in PAIR:
                a, b = AXES[c]
                wait(b2(p, c))
                de[unit(p, c), me[a] * 4 + me[b]] += rb2[c, k, 0] + rb2[c, k, 1]

        def col(b, dy, dx):
            dst = at("y", dy) * 4 + at("x", dx)
            return remote(sb.at[b, dst], rv.at[b, yi * 4 + xi], ass.at[b, dy * 4 + dx], asr.at[b, dy * 4 + dx], {"y": at("y", dy), "x": at("x", dx)})

        def col_arrive(b, dy, dx):
            src = at("y", -dy % 4) * 4 + at("x", -dx % 4)
            return remote(sb.at[b, src], rv.at[b, src], ass.at[b, dy * 4 + dx], asr.at[b, dy * 4 + dx], {"y": at("y", dy), "x": at("x", dx)})

        def out_de(b, x):
            lanes = pl.ds(x * VB + b * 4 * EC, 4 * EC)
            return pltpu.make_async_copy(de_s.at[:, lanes], de_out.at[:, lanes], desem.at[b, x])

        def do_cols(b):
            for k in QUAD:
                first, second = AXES[k % 2]
                mine = me[first] * 4 + me[second]
                for s in range(16):
                    sb[b, s, span(k, OWN), :] = de[4 * b + k, mine, span(s, OWN), :]
            start([col(b, dy, dx) for dy, dx in FAR])
            rv[b, yi * 4 + xi] = sb[b, yi * 4 + xi]

        def do_assemble(b):
            arrive([col_arrive(b, dy, dx) for dy, dx in FAR])
            for s in range(16):
                for k in QUAD:
                    lane = (s % 4) * VB + (4 * b + k) * EC + (s // 4) * LANE
                    de_s[:, pl.ds(lane, LANE)] = rv[b, s, span(k, OWN), :]
            start([out_de(b, x) for x in QUAD])

        def dcopy(r):
            return remote(dz.at[other, r], uf.at[r], dps.at[r], dpr.at[r], {"tp": other})

        def unit_in(r, q):
            return pltpu.make_async_copy(uf_out.at[2 * r + core, q], gst.at[q], gsem.at[q])

        def fetch(r):
            start([unit_in(r, q) for q in PAIR])

        def core_sum(r):
            dcopy(r).wait_recv()
            for q in PAIR:
                dz[core, r, q] += uf[r, q]

        def gain_sum(r):
            wait([unit_in(r, q) for q in PAIR])
            dg = gain[...]
            for q in PAIR:
                for j in PAIR:
                    dg = dg + dz[core, r, q, :, span(j, LANE)] * gst[q, :, span(j, LANE)]
            gain[...] = dg

        def c1(i, q):
            return remote(dz.at[core, 3, q, pl.ds(HD * i, HD)], uf.at[6, i, pl.ds(HD * q, HD)], c1s.at[i, q], c1r.at[i, q], hop("x", i))

        def c2(i):
            return remote(dz.at[core, 2 - i], uf.at[4 + i], c2s.at[i], c2r.at[i], hop("x", i))

        def far_unit(u, _):
            @pl.when(u == 2)
            def _():
                for i, (r, q) in enumerate(FIRST):
                    gmine[i].wait_recv()
                    gonward[i].start()
                    gpcopy(r, q).start()

            @pl.when(u == 4)
            def _():
                arrive([gparrive(r, q) for r, q in FIRST])
                start([stage_in(p) for p in PAIR])

            @pl.when(u == 8)
            def _():
                for i, (r, q) in enumerate(LATER):
                    gmine[2 + i].wait_recv()
                    gpcopy(r, q).start()

            @pl.when(u == 10)
            def _():
                arrive([gparrive(r, q) for r, q in LATER])
                start([stage_in(4 + p) for p in PAIR])

            @pl.when((u >= 5) & (u < 9))
            def _():
                convert(u - 5)

            @pl.when((u >= 5) & (u < 7))
            def _():
                stage_in(u - 3).start()

            @pl.when(u == 11)
            def _():
                convert(4)
                stage_in(6).start()

            far_step(u)
            return 0

        lax.fori_loop(0, 2 * NP, far_unit, 0)
        dcopy(3).start()

        def near_chunk(vc, _):
            @pl.when(vc == 0)
            def _():
                convert(5)
                stage_in(7).start()

            @pl.when((vc >= 1) & (vc < 3))
            def _():
                convert(vc + 5)

            @pl.when(vc == 2)
            def _():
                core_sum(3)
                start([c1(i, q) for i in PAIR for q in PAIR])

            @pl.when(vc == 3)
            def _():
                for i in PAIR:
                    gonward[i].wait_recv()
                    gpcopy(3, i).start()

            near_step(vc)
            return 0

        lax.fori_loop(0, NA, near_chunk, 0)
        arrive([gparrive(3, i) for i in PAIR])
        start([stage_in(8 + p) for p in PAIR])
        for p in range(8, 12):
            convert(p)
            if p < 10:
                stage_in(p + 2).start()

        def phase_c(p, _):
            @pl.when(p >= 1)
            def _():
                do_a2(p - 1)

            lookups(4 * p)

            @pl.when(p >= 2)
            def _():
                do_b2(p - 2)

            do_a1(p)

            @pl.when(p == 4)
            def _():
                do_cols(0)

            def more(i, _):
                near_step(NA + 4 * p + i)
                return 0

            lax.fori_loop(0, 4, more, 0)

            @pl.when(p >= 2)
            def _():
                do_f(p - 2)

            @pl.when(p >= 1)
            def _():
                do_b1(p - 1)

            return 0

        lax.fori_loop(0, NP - 1, phase_c, 0)

        start([dcopy(r) for r in (1, 2)])
        fetch(1)
        for slot in PAIR:
            start(far_load(slot, 0))
        do_a2(4)
        gain[...] = jnp.zeros_like(gain)

        def to_neighbour(i):
            core_sum(2 - i)
            for q in PAIR:
                c1(i, q).wait()
                dz[core, 2 - i, q, span(i, HD)] += uf[6, i, span(q, HD)]
            c2(i).start()

        def last_lookups(i, _):
            lookup_step(20 + i)

            @pl.when(i == 0)
            def _():
                to_neighbour(1)

            @pl.when(i == 1)
            def _():
                to_neighbour(0)

            @pl.when(i == 2)
            def _():
                gain_sum(1)
                fetch(2)

            return 0

        lax.fori_loop(0, 4, last_lookups, 0)
        do_b2(3)
        do_a1(5)

        def own_unit(u, _):
            @pl.when(u == 1)
            def _():
                do_b1(4)

            @pl.when(u == 2)
            def _():
                gain_sum(2)
                fetch(0)

            @pl.when(u == 5)
            def _():
                do_b2(4)
                do_a2(5)

            @pl.when(u == 8)
            def _():
                do_f(3)
                do_cols(1)

            own_step(u)
            return 0

        lax.fori_loop(0, 2 * NP, own_unit, 0)
        dcopy(0).start()
        do_f(4)
        core_sum(0)
        gain_sum(0)
        st[core] = jnp.zeros(SUMS, F32)
        st[core, ROW0, span(0, D)] = jnp.sum(gain[...].T, axis=0, keepdims=True)
        st[core, ROW1, span(0, TB)] = aux[0, ROW1, :]
        pair_copy = remote(st.at[core], st.at[core], sts, str_, {"tp": other})
        pair_arrive = remote(st.at[core], st.at[other], sts, str_, {"tp": other})
        pair_copy.start()
        sums = [gather_axis(buf, axis, sas.at[k], sar.at[k]) for k, (buf, axis) in enumerate(((sz, "z"), (sy, "y"), (sx, "x")))]
        do_b1(5)
        pair_arrive.wait()
        sz[zi] = st[0] + st[1]
        start(sums[0][0])
        do_assemble(0)
        do_b2(5)
        wait(sums[0][1])
        sy[yi] = sum4(sz)
        start(sums[1][0])
        do_f(5)
        do_cols(2)
        wait(sums[1][1])
        sx[xi] = sum4(sy)
        start(sums[2][0])
        do_assemble(1)

        for q in PAIR:
            rows = h_ref[:, pl.ds(pl.multiple_of(core * TS + q * TB, TB), TB)].astype(F32)
            inv = lax.rsqrt(jnp.mean(rows * rows, axis=0, keepdims=True) + RMS_EPS)
            gst[q] = rows * inv
            aux[q, ROW0, :] = inv
        wait([c2(i) for i in PAIR])
        for q in PAIR:
            unit, inv = gst[q], aux[q, ROW0, :]
            gu = (dz[core, 0, q] + uf[4, q] + uf[5, q]) * weight
            dz[core, 3, q] = inv * (gu - unit * jnp.mean(gu * unit, axis=0, keepdims=True))
        half_copy = remote(dz.at[core, 3], uf.at[7], hs, hr, {"tp": other})
        half_copy.start()
        wait(sums[2][1])
        sum_out[...] = sum4(sx)
        sum_out[ROW1, span(0, TB)] = sum_out[ROW1, span(0, TB)] / aux[1, ROW1, :]
        half_copy.wait()
        for half in PAIR:
            for q in PAIR:
                gb[half, q] = jnp.where(core == half, dz[core, 3, q], uf[7, q]).astype(BF16)
                out_dh(half, q).start()
        do_assemble(2)
        wait([out_dh(half, q) for half in PAIR for q in PAIR])
        wait([out_de(b, x) for b in BATCHES for x in QUAD])

        sent(gmine + gonward + [gpcopy(r, q) for r in HOPS for q in PAIR] + [dcopy(r) for r in QUAD])
        sent([col(b, dy, dx) for b in BATCHES for dy, dx in FAR])
    pl.run_scoped(
        backward, V((2, GX, 2, D, TB), F32), V((2 * NP, 16, ROWS, LANE), F32), V((2, NS, V2, TS), F32), V((2, D, EC), BF16)
    )
    sent([icopy(d) for d in HOPS] + ny_out + nz_out)
    for r in QUAD:
        sent(stat_copies(r))


def call(*args):
    links = [DMA((2, 2, 2))] * 8
    return pl.pallas_call(
        kernel,
        out_shape=(
            SDS((OWN, VL), F32), SDS((D, TOK), BF16), SDS(SUMS, F32),
            SDS((NS, VB, TS), F32), SDS(TOKENS, F32), SDS(TOKENS, F32),
        ),
        in_specs=[VMEM, ANY] + [VMEM] * 4 + [ANY],
        out_specs=(ANY, ANY, VMEM) + (ANY,) * 3,
        scratch_shapes=[
            V(TOKENS, F32),
            *[V(TOKENS, BF16)] * 2,
            V((2, D, TB), F32),
            V((GX, 2, 2, SUB, TB), I32),
            V((NS, GX, SUB, TB), F32), V((1, TB), F32),
            *[V((GX, SUB, LANE), F32)] * 2,
            V((NS, 2, TS), F32), V((NS, 2, TS), I32), V((2, SUB, TB), F32),
            V((D, LANE), F32),
            V((OWN, VL), F32),
            V((2, 2, 2, 2, ROWS, LANE), F32),
            V((2, 2, 2, GX, ROWS, LANE), F32),
            V((2, 2, 2, HROWS, LANE), F32),
            V((2, 2, 2, ROWS, LANE), F32),
            *[V((3, 16, 40, LANE), F32)] * 2,
            V((2, *SUMS), F32), *[V((GX, *SUMS), F32)] * 3,
            DMA((3, GX)), DMA((2 * NP,)), DMA((2,)), DMA((2, 2)), *[DMA((2,))] * 2, DMA((2, 2)), *[DMA((NS, 2))] * 2,
            DMA((NS,)), *[DMA((GX, 2))] * 3, *[DMA((GX,))] * 2, *[DMA((NS, GX))] * 2, *[DMA((2, GX))] * 2,
            DMA((NS,)), *[DMA((GX, 2))] * 3, *links,
            *[DMA((3, 16))] * 2, *[DMA((GX,))] * 2, *[DMA((2, 2))] * 2, *[DMA((2,))] * 2, *[DMA(())] * 4, *[DMA((3, GX))] * 2,
        ],
        compiler_params=pltpu.CompilerParams(vmem_limit_bytes=67043328, collective_id=0, has_side_effects=True),
    )(*args)


def solution(mesh):
    mesh4 = Mesh(mesh.devices.reshape(2, GX, GX, GX), ("tp", "z", "y", "x"))

    def local_step(hidden, norm_w, embed, targets, loss_mask, token_ids, grad_embed):
        h_t = hidden.reshape(TOK, D).T
        ge_t = grad_embed.reshape(TOK, D).T
        de, dh, sums, *_ = call(h_t, ge_t, norm_w.reshape(D, 1), targets, loss_mask, token_ids, embed.T)
        return sums[1, 0], dh.T.reshape(hidden.shape), sums[0, :D], de.T

    dp = ("z", "y", "x")
    return jax.shard_map(
        local_step,
        mesh=mesh4,
        in_specs=(P(dp), P(), P("tp"), P(dp), P(dp), P(dp), P(dp)),
        out_specs=(P(), P(dp), P(), P("tp", dp)),
        check_vma=False,
    )
```
